32 devices in a mesh: row: 8 (over z, y), col: 4 (over x, core).
Axes of the slice: x: 2, y: 2, z: 4, core: 2. Of those that a mesh axis runs over, the one named last changes fastest.
Arguments:
- eigvecs: float32 [32768, 512], P('row', 'col'), may hold values from -6 to 6
- reflectors: float32 [2, 32768, 512], P(None, 'row', 'col'), may hold values from -0.03125 to 0.03125
- factors: float32 [2, 512, 512], replicated, may hold values from -1 to 2, as said below
- slab: float32 [2048, 32768], P('col', 'row'), may hold values from -0.03125 to 0.03125
Outputs:
- vectors: float32 [32768, 512], P('row', 'col')
- product: float32 [2048, 512], P('col', 'row')
The draws below stay inside these ranges and needn't reach their ends.
Inputs may be any that keep to these rules, and one draw needn't show every extreme that they name: Each of the two 512 x 512 factors is upper triangular, with diagonal entries between 1 and 2.
All inputs are finite; a program needn't handle non-finite values.
Results may differ from the reference program's by a relative error of at most 0.000088.
Values sent between devices are 32-bit elements; how exact they have to be, the bound alone decides.
A program may use at most 128 MiB of HBM per device.

```python
import jax
import jax.numpy as jnp
from jax import lax

N = 32768
B = 512
K = 512
SLAB = 2048


def draw_factors(key, part):
    upper_key = jax.random.fold_in(key, 11)
    diag_key = jax.random.fold_in(key, 23)
    upper = jax.random.normal(upper_key, (2, B, B), jnp.float32) / jnp.sqrt(jnp.float32(B))
    diag = jax.random.uniform(diag_key, (2, B), jnp.float32, 1.0, 2.0)
    upper = jnp.clip(upper, -0.9, 0.9)
    rows = lax.broadcasted_iota(jnp.int32, (2, B, B), 1)
    cols = lax.broadcasted_iota(jnp.int32, (2, B, B), 2)
    strict = jnp.where(cols > rows, upper, jnp.float32(0.0))
    return jnp.where(cols == rows, diag[:, :, None], strict)


def level_of(own_key, shape, cuts, smallest, top_value):
    gain, own = 1.0, jax.random.fold_in(own_key, 6)
    for dim, blocks in cuts:
        draws = jnp.exp(jax.random.uniform(jax.random.fold_in(own, dim), (blocks,), jnp.float32, smallest / len(cuts), top_value / len(cuts)))
        gain = gain * jnp.repeat(draws, shape[dim] // blocks).reshape([-1 if axis == dim else 1 for axis in range(len(shape))])
    return gain


def scatter_about(rng, shape, width, reach, shards=(), dtype=jnp.bfloat16):
    array = jax.random.normal(rng, shape, jnp.float32) * width
    if len(shards) > 0:
        array = level_of(rng, shape, shards, -0.22, 0.18) * array
    return jnp.clip(array, min=-reach, max=reach).astype(dtype)


def setup_inputs(seed: int = 0) -> dict:
    key_of = jax.random.split(jax.random.key(seed), 5)
    eigvecs = scatter_about(key_of[0], (N, K), 1.0, 6.0, ((0, 8), (1, 4)), jnp.float32)
    reflectors = scatter_about(key_of[1], (2, N, B), N ** -0.5, 0.03125, ((1, 8), (2, 4)), jnp.float32)
    factors = draw_factors(jax.random.fold_in(key_of[4], 71), 0)
    slab = scatter_about(key_of[3], (SLAB, N), N ** -0.5, 0.03125, ((0, 4), (1, 8)), jnp.float32)
    return dict(eigvecs=eigvecs, reflectors=reflectors, factors=factors, slab=slab)


def matmul(left, right):
    return jnp.dot(left, right, precision=lax.Precision.HIGHEST, preferred_element_type=jnp.float32)


def reference(eigvecs, reflectors, factors, slab):
    first_y = reflectors[0]
    second_y = reflectors[1]
    second_w = matmul(second_y.T, eigvecs)
    inner = eigvecs - matmul(matmul(second_y, factors[1]), second_w)
    first_w = matmul(first_y.T, inner)
    vectors = inner - matmul(matmul(first_y, factors[0]), first_w)
    product = matmul(slab, vectors)
    return vectors, product
```

```python
import functools

import jax
import jax.numpy as jnp
from jax import lax
from jax.experimental import pallas as pl
from jax.experimental.pallas import tpu as pltpu
from jax.sharding import PartitionSpec as P

MESH = pl.DeviceIdType.MESH
NN = ((1,), (0,))
NT = ((1,), (1,))
TN = ((0,), (0,))


def dot(left, right, dims=NN):
    return lax.dot_general(
        left, right, (dims, ((), ())), precision=lax.Precision.HIGH, preferred_element_type=jnp.float32
    )


def tdot(left, right):
    return dot(left, right, TN)


def halves(a):
    high = a.astype(jnp.bfloat16)
    return high, (a - high.astype(jnp.float32)).astype(jnp.bfloat16)


def dot3(left, right, dims):
    def one(a, b):
        return lax.dot_general(a, b, (dims, ((), ())), preferred_element_type=jnp.float32)

    (lh, ll), (rh, rl) = left, right
    return one(lh, rh) + (one(lh, rl) + one(ll, rh))


def loop(lo, hi, body):
    if hi - lo == 1:
        body(lo)
    elif hi > lo:
        lax.fori_loop(lo, hi, lambda i, carry: (body(i), carry)[1], 0)


def aligned(i, size):
    return pl.ds(pl.multiple_of(i * size, size), size)


def whole_kernel(
    dims, x_hbm, y_hbm, t_hbm, s_hbm, vec_hbm, out_ref,
    xb, y1b, y2b, sb, tb, vb, w, wf, tw, ybuf, zbuf, xs, xr, pacc, pt, pyb, pzb,
    lx, ly, ls, px_s, px_r, py_s, py_r, m_s, m_r, f_s, f_r,
    ry_s, ry_r, rz_s, rz_r, rx_s, rx_r, gz_s, gz_r, gy_s, gy_r,
    vp_s, vp_r, vm_s, vm_r, vo,
):
    nz, q, nq, early, late = dims
    extra = early + late
    held = nq + extra
    bw = x_hbm.shape[1]
    r, c = lax.axis_index("row"), lax.axis_index("col")
    z, y = r // 2, lax.rem(r, 2)
    x, k = c // 2, lax.rem(c, 2)
    mate = (r, c + 1 - 2 * k)
    peer = (r, c + 2 - 4 * x)
    peer_block = c + 2 - 4 * x
    ynext = (r + 1 - 2 * y, c)

    def zat(d):
        return lax.rem(z + d, nz)

    def znext(d):
        return (zat(d) * 2 + y, c)

    partners = [mate, peer, ynext] + [znext(d) for d in range(1, nz)]
    barrier = pltpu.get_barrier_semaphore()
    for other in partners:
        pl.semaphore_signal(barrier, inc=1, device_id=other, device_id_type=MESH)
    pl.semaphore_wait(barrier, len(partners))

    def send(src, dst, s, t, device):
        return pltpu.make_async_remote_copy(src, dst, s, t, device_id=device, device_id_type=MESH)

    def chunk(i):
        return aligned(i, q)

    def place(i, side):
        within = lax.rem(i, nq)
        half = jnp.where(i < nq, side, 1 - side)
        return pl.ds(pl.multiple_of((half * nq + within) * q, q), q)

    def lanes(b):
        return aligned(b, bw)

    panels = (y1b, y2b)

    def x_local(i):
        return pltpu.make_async_copy(x_hbm.at[place(i, x)], xb.at[chunk(i), lanes(x)], lx.at[i])

    def x_peer(i):
        return send(x_hbm.at[place(i, 1 - x)], xb.at[chunk(i), lanes(x)], px_s.at[i], px_r.at[i], peer)

    def y_local(p, i):
        return pltpu.make_async_copy(y_hbm.at[p, place(i, x)], panels[p].at[chunk(i), lanes(c)], ly.at[p, i])

    def y_peer(p, i):
        return send(
            y_hbm.at[p, place(i, 1 - x)], panels[p].at[chunk(i), lanes(c)], py_s.at[p, i], py_r.at[p, i], peer)

    def y_mate(p, i):
        return send(y_hbm.at[p, place(i, x)], panels[p].at[chunk(i), lanes(c)], m_s.at[p, i], m_r.at[p, i], mate)

    def y_forward(p, i):
        block = panels[p].at[chunk(i), lanes(peer_block)]
        return send(block, block, f_s.at[p, i], f_r.at[p, i], mate)

    def wait_x(i):
        x_local(i).wait()
        x_peer(i).wait_recv()

    def wait_y(p, i):
        y_local(p, i).wait()
        y_mate(p, i).wait_recv()
        y_forward(p, i).wait_recv()

    def pass_on(p, i):
        y_peer(p, i).wait_recv()
        y_forward(p, i).start()

    def send_bulk(i):
        x_peer(i).start()
        y_peer(1, i).start()
        y_peer(0, i).start()

    def first_two(i):
        x_peer(i).start()
        y_peer(1, i).start()

    loop(0, nq, first_two)
    loop(0, nq, lambda i: y_peer(0, i).start())

    def own(i):
        x_local(i).start()
        y_mate(1, i).start()
        y_local(1, i).start()
        y_mate(0, i).start()
        y_local(0, i).start()

    loop(0, held, own)
    t_copy = pltpu.make_async_copy(t_hbm, tb, ls.at[0])
    s_copy = pltpu.make_async_copy(s_hbm, sb, ls.at[1])
    t_copy.start()
    s_copy.start()

    w[...] = jnp.zeros_like(w)
    pacc[...] = jnp.zeros_like(pacc)

    def step(i):
        @pl.when(i < nq)
        def _():
            pass_on(1, i)

        @pl.when(i > 0)
        def _():
            j = i - 1
            wait_x(j)
            wait_y(1, j)
            w[0] += dot3(halves(xb[chunk(j), :]), halves(y2b[chunk(j), :]), TN)

    loop(0, nq + 1, step)
    t_copy.wait()
    s_copy.wait()

    rows = w.shape[1] // (2 * nz)

    def sum_rows(n, piece, ys, zs):
        order = list(range(1, nz)) + [0]
        out = [send(piece(zat(d), 1 - y), ys.at[d], ry_s.at[n, d], ry_r.at[n, d], ynext) for d in order]
        for copy in out:
            copy.start()
        hops = []
        for d, copy in zip(order, out):
            copy.wait_recv()
            mine = piece(zat(d), y)
            if d:
                mine[...] += ys[d]
                hops.append(send(mine, zs.at[d], rz_s.at[n, d], rz_r.at[n, d], znext(d)))
                hops[-1].start()
            else:
                total = mine[...] + ys[0]
        for d, copy in zip(order, hops):
            copy.wait_recv()
            total = total + zs[d]
        return total, out + hops

    def all_sum(n, after_exchange, before_last):
        def piece(zz, yy):
            return w.at[n, aligned(zz * 2 + yy, rows)]

        def final(zz, yy):
            return wf.at[n, aligned(zz * 2 + yy, rows)]

        total, sent = sum_rows(n, piece, ybuf.at[n], zbuf.at[n])
        xs[n] = total
        swap = send(xs.at[n], xr.at[n], rx_s.at[n], rx_r.at[n], peer)
        swap.start()
        after_exchange()
        swap.wait_recv()
        mine = final(z, y)
        mine[...] = xs[n] + xr[n]
        along = [send(mine, mine, gz_s.at[n, d], gz_r.at[n, d], znext(d)) for d in range(1, nz)]
        for copy in along:
            copy.start()
        across = [send(mine, mine, gy_s.at[n, 0], gy_r.at[n, 0], ynext)]
        across[0].start()
        for d in range(1, nz):
            along[d - 1].wait_recv()
            block = final(lax.rem(z + nz - d, nz), y)
            across.append(send(block, block, gy_s.at[n, d], gy_r.at[n, d], ynext))
            across[-1].start()
        before_last()
        for copy in across:
            copy.wait_recv()
        return sent + [swap] + along + across

    def inner(i):
        xb[chunk(i), :] = xb[chunk(i), :] - dot3(halves(y2b[chunk(i), :]), halves(tw[1]), NN)

    def apply(p, n):
        tw[p] = dot3(halves(tb[p]), halves(wf[n]), NT)

    sent = all_sum(0, lambda: loop(nq, nq + early, send_bulk), lambda: loop(0, nq, lambda i: pass_on(0, i)))
    apply(1, 0)

    def second(i):
        inner(i)
        wait_y(0, i)
        w[1] += dot3(halves(xb[chunk(i), :]), halves(y1b[chunk(i), :]), TN)

    loop(0, nq, second)

    def take_extra(i):
        pass_on(1, i)
        pass_on(0, i)

    def extra_inner(i):
        wait_x(i)
        wait_y(1, i)
        inner(i)

    def early_extra():
        loop(nq, nq + early, take_extra)
        loop(nq, nq + early, extra_inner)

    sent += all_sum(1, lambda: loop(nq + early, held, send_bulk), early_extra)
    apply(0, 1)

    def v_mate(i):
        block = vb.at[k, chunk(i)]
        return send(block, block, vm_s.at[i], vm_r.at[i], mate)

    def v_peer(i):
        return send(vb.at[k, chunk(i)], vb.at[k, chunk(i + nq)], vp_s.at[i], vp_r.at[i], peer)

    def v_out(i):
        return pltpu.make_async_copy(vb.at[k, chunk(i), lanes(x)], vec_hbm.at[place(i, x)], vo.at[i])

    def finish(i):
        vb[k, chunk(i), :] = xb[chunk(i), :] - dot3(halves(y1b[chunk(i), :]), halves(tw[0]), NN)

    def ship(i):
        v_mate(i).start()
        v_out(i).start()

    def finish_sent(i):
        finish(i)
        v_peer(i).start()
        ship(i)

    def finish_kept(i):
        finish(i)
        ship(i)

    def finish_extra(i):
        wait_y(0, i)
        finish(i)
        ship(i)

    loop(extra, nq, finish_sent)
    loop(nq + early, held, take_extra)
    loop(0, extra, finish_kept)
    loop(nq + early, held, extra_inner)
    loop(nq, held, finish_extra)

    def columns(i):
        return halves(sb[:, place(i, x)])

    def multiply(i):
        v_mate(i).wait_recv()
        part = columns(i)
        for h in range(2):
            pacc[h] += dot3(part, halves(vb[h, chunk(i), :]), NN)

    def multiply_far(i):
        v_peer(i - nq).wait_recv()
        ship(i)
        part = columns(i)
        pacc[k] += dot3(part, halves(vb[k, chunk(i), :]), NN)
        v_mate(i).wait_recv()
        pacc[1 - k] += dot3(part, halves(vb[1 - k, chunk(i), :]), NN)

    loop(0, held, multiply)
    loop(held, 2 * nq, multiply_far)

    for h in range(2):
        for side in range(2):
            pt[h + 2 * side] = pacc[h, :, side * bw : (side + 1) * bw].T

    share = out_ref.shape[0]
    total, last = sum_rows(2, lambda zz, yy: pt.at[zz, aligned(yy, share)], pyb, pzb)
    out_ref[...] = total

    for copy in sent + last:
        copy.wait_send()

    def drain(i):
        x_peer(i).wait_send()
        for p in range(2):
            y_peer(p, i).wait_send()
            y_mate(p, i).wait_send()
            y_forward(p, i).wait_send()

    loop(0, held, drain)
    loop(extra, nq, lambda i: v_peer(i).wait_send())

    def drain_v(i):
        v_mate(i).wait_send()
        v_out(i).wait()

    loop(0, 2 * nq, drain_v)


CHUNK = 512
EARLY, LATE = 1, 1


def on_grid(nrow, ncol, eigvecs, reflectors, factors, slab):
    size, bw = eigvecs.shape
    panel = factors.shape[1]
    nz = nrow // 2
    half = size // 2
    q = min(CHUNK, half)
    nq = half // q
    early, late = min(EARLY, nq), min(LATE, nq - min(EARLY, nq))
    extra = early + late
    held = nq + extra
    kept = held * q
    wide = 2 * bw
    f32 = jnp.float32
    rows = wide // nrow
    mine = slab.shape[0]
    share = ncol * bw // nrow
    sem = pltpu.SemaphoreType.DMA
    vmem = pltpu.VMEM
    vectors, product = pl.pallas_call(
        functools.partial(whole_kernel, (nz, q, nq, early, late)),
        out_shape=(
            jax.ShapeDtypeStruct((size, bw), f32),
            jax.ShapeDtypeStruct((share, mine), f32),
        ),
        in_specs=[pl.BlockSpec(memory_space=pl.ANY)] * 4,
        out_specs=(pl.BlockSpec(memory_space=pl.ANY), pl.BlockSpec(memory_space=pltpu.VMEM)),
        scratch_shapes=[
            vmem((kept, wide), f32), vmem((kept, panel), f32), vmem((kept, panel), f32),
            vmem(slab.shape, f32), vmem(factors.shape, f32), vmem((2, size, wide), f32),
            vmem((2, wide, panel), f32), vmem((2, wide, panel), f32), vmem((2, panel, wide), f32),
            vmem((2, nz, rows, panel), f32), vmem((2, nz, rows, panel), f32),
            vmem((2, rows, panel), f32), vmem((2, rows, panel), f32),
            vmem((2, mine, wide), f32), vmem((nz, bw, mine), f32),
            vmem((nz, share, mine), f32), vmem((nz, share, mine), f32),
            sem((held,)), sem((2, held)), sem((2,)),
            sem((held,)), sem((held,)), sem((2, held)), sem((2, held)),
            sem((2, held)), sem((2, held)), sem((2, held)), sem((2, held)),
            sem((3, nz)), sem((3, nz)), sem((3, nz)), sem((3, nz)),
            sem((2,)), sem((2,)),
            sem((2, nz)), sem((2, nz)), sem((2, nz)), sem((2, nz)),
            sem((nq,)), sem((nq,)), sem((2 * nq,)), sem((2 * nq,)), sem((2 * nq,)),
        ],
        compiler_params=pltpu.CompilerParams(
            collective_id=0, has_side_effects=True, vmem_limit_bytes=66_000_000),
        name="whole",
    )(eigvecs, reflectors, factors, slab)
    return vectors, product.T


def on_any(nrow, ncol, eigvecs, reflectors, factors, slab):
    c = lax.axis_index("col")
    first_own, second_own = reflectors[0], reflectors[1]
    all_x, second_y, first_y = (
        lax.all_gather(block, "col", axis=1, tiled=True) for block in (eigvecs, second_own, first_own)
    )
    own = second_own.shape[1]
    both = jnp.concatenate([second_own, first_own], axis=1)
    stacked = jnp.concatenate([tdot(both, all_x), tdot(first_own, second_y)])
    slab_x, slab_second, slab_first = (dot(block, slab, ((0,), (1,))) for block in (all_x, second_y, first_y))
    sums = lax.all_gather(lax.psum(stacked, "row"), "col")
    panel = factors.shape[1]
    second_w, first_raw, gram = (sums[:, i * own : (i + 1) * own].reshape(panel, -1) for i in range(3))
    second_tw = dot(factors[1], second_w)
    first_tw = dot(factors[0], first_raw - dot(gram, second_tw))
    partial = slab_x - tdot(second_tw, slab_second) - tdot(first_tw, slab_first)
    product = lax.psum_scatter(partial, "row", tiled=True)
    vectors = eigvecs
    for block, tw in ((second_y, second_tw), (first_y, first_tw)):
        width = eigvecs.shape[1]
        vectors = vectors - dot(block, lax.dynamic_slice_in_dim(tw, c * width, width, axis=1))
    return vectors, product.T


def solution(mesh):
    nrow, ncol = mesh.shape["row"], mesh.shape["col"]
    fits = ncol == 4 and nrow == 2 * ncol
    return jax.shard_map(
        functools.partial(on_grid if fits else on_any, nrow, ncol),
        mesh=mesh,
        in_specs=(P("row", "col"), P(None, "row", "col"), P(), P("col", "row")),
        out_specs=(P("row", "col"), P("col", "row")),
        check_vma=False,
    )
```

```python
import functools

import jax
import jax.numpy as jnp
from jax import lax
from jax.experimental import pallas as pl
from jax.experimental.pallas import tpu as pltpu
from jax.sharding import PartitionSpec as P

MESH = pl.DeviceIdType.MESH
NN = ((1,), (0,))
NT = ((1,), (1,))
TN = ((0,), (0,))


def dot(left, right, dims=NN):
    return lax.dot_general(
        left, right, (dims, ((), ())), precision=lax.Precision.HIGH, preferred_element_type=jnp.float32
    )


def tdot(left, right):
    return dot(left, right, TN)


def halves(a):
    high = a.astype(jnp.bfloat16)
    return high, (a - high.astype(jnp.float32)).astype(jnp.bfloat16)


def dot3(left, right, dims):
    def one(a, b):
        return lax.dot_general(a, b, (dims, ((), ())), preferred_element_type=jnp.float32)

    (lh, ll), (rh, rl) = left, right
    return one(lh, rh) + (one(lh, rl) + one(ll, rh))


def loop(lo, hi, body):
    if hi - lo == 1:
        body(lo)
    elif hi > lo:
        lax.fori_loop(lo, hi, lambda i, carry: (body(i), carry)[1], 0)


def aligned(i, size):
    return pl.ds(pl.multiple_of(i * size, size), size)


def whole_kernel(
    dims, x_hbm, y_hbm, t_hbm, s_hbm, vec_hbm, out_ref,
    xb, y1b, y2b, sb, tb, vb, w, gram, wf, tw, ybuf, zbuf, xs, xr, pacc, pt, pyb, pzb,
    lx, ly, ls, px_s, px_r, py_s, py_r, m_s, m_r, f_s, f_r,
    ry_s, ry_r, rz_s, rz_r, rx_s, rx_r, gz_s, gz_r, gy_s, gy_r,
    vp_s, vp_r, vm_s, vm_r, vo,
):
    nz, q, nq, ahead, early, late = dims
    extra = early + late
    held = nq + extra
    bw = x_hbm.shape[1]
    r, c = lax.axis_index("row"), lax.axis_index("col")
    z, y = r // 2, lax.rem(r, 2)
    x, k = c // 2, lax.rem(c, 2)
    mate = (r, c + 1 - 2 * k)
    peer = (r, c + 2 - 4 * x)
    peer_block = c + 2 - 4 * x
    ynext = (r + 1 - 2 * y, c)

    def zat(d):
        return lax.rem(z + d, nz)

    def znext(d):
        return (zat(d) * 2 + y, c)

    partners = [mate, peer, ynext] + [znext(d) for d in range(1, nz)]
    barrier = pltpu.get_barrier_semaphore()
    for other in partners:
        pl.semaphore_signal(barrier, inc=1, device_id=other, device_id_type=MESH)
    pl.semaphore_wait(barrier, len(partners))

    def send(src, dst, s, t, device):
        return pltpu.make_async_remote_copy(src, dst, s, t, device_id=device, device_id_type=MESH)

    def chunk(i):
        return aligned(i, q)

    def place(i, side):
        within = lax.rem(i, nq)
        half = jnp.where(i < nq, side, 1 - side)
        return pl.ds(pl.multiple_of((half * nq + within) * q, q), q)

    def lanes(b):
        return aligned(b, bw)

    panels = (y1b, y2b)

    def x_local(i):
        return pltpu.make_async_copy(x_hbm.at[place(i, x)], xb.at[chunk(i), lanes(x)], lx.at[i])

    def x_peer(i):
        return send(x_hbm.at[place(i, 1 - x)], xb.at[chunk(i), lanes(x)], px_s.at[i], px_r.at[i], peer)

    def y_local(p, i):
        return pltpu.make_async_copy(y_hbm.at[p, place(i, x)], panels[p].at[chunk(i), lanes(c)], ly.at[p, i])

    def y_peer(p, i):
        return send(
            y_hbm.at[p, place(i, 1 - x)], panels[p].at[chunk(i), lanes(c)], py_s.at[p, i], py_r.at[p, i], peer)

    def y_mate(p, i):
        return send(y_hbm.at[p, place(i, x)], panels[p].at[chunk(i), lanes(c)], m_s.at[p, i], m_r.at[p, i], mate)

    def y_forward(p, i):
        block = panels[p].at[chunk(i), lanes(peer_block)]
        return send(block, block, f_s.at[p, i], f_r.at[p, i], mate)

    def wait_x(i):
        x_local(i).wait()
        x_peer(i).wait_recv()

    def wait_y(p, i):
        y_local(p, i).wait()
        y_mate(p, i).wait_recv()
        y_forward(p, i).wait_recv()

    def pass_on(p, i):
        y_peer(p, i).wait_recv()
        y_forward(p, i).start()

    def send_bulk(i):
        x_peer(i).start()
        y_peer(1, i).start()
        y_peer(0, i).start()

    def first_two(i):
        x_peer(i).start()
        y_peer(1, i).start()

    loop(0, nq, first_two)
    loop(0, ahead, lambda i: y_peer(0, i).start())

    def own(i):
        x_local(i).start()
        y_mate(1, i).start()
        y_local(1, i).start()
        y_mate(0, i).start()
        y_local(0, i).start()

    loop(0, held, own)
    t_copy = pltpu.make_async_copy(t_hbm, tb, ls.at[0])
    s_copy = pltpu.make_async_copy(s_hbm, sb, ls.at[1])
    t_copy.start()
    s_copy.start()

    w[...] = jnp.zeros_like(w)
    gram[...] = jnp.zeros_like(gram)
    pacc[...] = jnp.zeros_like(pacc)

    def step(i):
        @pl.when(i < nq)
        def _():
            pass_on(1, i)

        @pl.when(i > 0)
        def _():
            j = i - 1
            wait_x(j)
            wait_y(1, j)
            w[0] += dot3(halves(xb[chunk(j), :]), halves(y2b[chunk(j), :]), TN)

    loop(0, nq + 1, step)
    t_copy.wait()
    s_copy.wait()

    rows = w.shape[1] // (2 * nz)

    def sum_rows(n, piece, ys, zs, meanwhile):
        order = list(range(1, nz)) + [0]
        out = [send(piece(zat(d), 1 - y), ys.at[d], ry_s.at[n, d], ry_r.at[n, d], ynext) for d in order]
        for copy in out:
            copy.start()
        hops = []
        for d, copy in zip(order, out):
            copy.wait_recv()
            mine = piece(zat(d), y)
            if d:
                mine[...] += ys[d]
                hops.append(send(mine, zs.at[d], rz_s.at[n, d], rz_r.at[n, d], znext(d)))
                hops[-1].start()
            else:
                total = mine[...] + ys[0]
        meanwhile()
        for d, copy in zip(order, hops):
            copy.wait_recv()
            total = total + zs[d]
        return total, out + hops

    def all_sum(n, meanwhile, after_exchange, after_sends, before_last):
        def piece(zz, yy):
            return w.at[n, aligned(zz * 2 + yy, rows)]

        def final(zz, yy):
            return wf.at[n, aligned(zz * 2 + yy, rows)]

        total, sent = sum_rows(n, piece, ybuf.at[n], zbuf.at[n], meanwhile)
        xs[n] = total
        swap = send(xs.at[n], xr.at[n], rx_s.at[n], rx_r.at[n], peer)
        swap.start()
        after_exchange()
        swap.wait_recv()
        mine = final(z, y)
        mine[...] = xs[n] + xr[n]
        along = [send(mine, mine, gz_s.at[n, d], gz_r.at[n, d], znext(d)) for d in range(1, nz)]
        for copy in along:
            copy.start()
        across = [send(mine, mine, gy_s.at[n, 0], gy_r.at[n, 0], ynext)]
        across[0].start()
        after_sends()
        for d in range(1, nz):
            along[d - 1].wait_recv()
            block = final(lax.rem(z + nz - d, nz), y)
            across.append(send(block, block, gy_s.at[n, d], gy_r.at[n, d], ynext))
            across[-1].start()
        before_last()
        for copy in across:
            copy.wait_recv()
        return sent + [swap] + along + across

    def inner(i):
        xb[chunk(i), :] = xb[chunk(i), :] - dot3(halves(y2b[chunk(i), :]), halves(tw[1]), NN)

    def apply(p, n):
        tw[p] = dot3(halves(tb[p]), halves(wf[n]), NT)

    def raw(i):
        wait_y(0, i)
        first = halves(y1b[chunk(i), :])
        w[1] += dot3(halves(xb[chunk(i), :]), first, TN)
        gram[...] += dot3(halves(y2b[chunk(i), :]), first, TN)

    def rest():
        loop(ahead, nq, lambda i: y_peer(0, i).start())
        loop(nq, nq + early, send_bulk)
        loop(0, nq - 2, lambda i: pass_on(0, i))
        loop(0, nq - 2, raw)

    def nearly():
        pass_on(0, nq - 2)
        raw(nq - 2)

    sent = all_sum(0, lambda: None, rest, nearly, lambda: pass_on(0, nq - 1))
    apply(1, 0)
    raw(nq - 1)
    w[1] = w[1] - dot3(halves(tw[1]), halves(gram[...]), TN)

    def take_extra(i):
        pass_on(1, i)
        pass_on(0, i)

    def extra_inner(i):
        wait_x(i)
        wait_y(1, i)
        inner(i)

    def early_extra():
        loop(nq, nq + early, take_extra)
        loop(nq, nq + early, extra_inner)

    sent += all_sum(
        1, lambda: loop(0, nq, inner), lambda: loop(nq + early, held, send_bulk), lambda: None, early_extra)
    apply(0, 1)

    def v_mate(i):
        block = vb.at[k, chunk(i)]
        return send(block, block, vm_s.at[i], vm_r.at[i], mate)

    def v_peer(i):
        return send(vb.at[k, chunk(i)], vb.at[k, chunk(i + nq)], vp_s.at[i], vp_r.at[i], peer)

    def v_out(i):
        return pltpu.make_async_copy(vb.at[k, chunk(i), lanes(x)], vec_hbm.at[place(i, x)], vo.at[i])

    def finish(i):
        vb[k, chunk(i), :] = xb[chunk(i), :] - dot3(halves(y1b[chunk(i), :]), halves(tw[0]), NN)

    def ship(i):
        v_mate(i).start()
        v_out(i).start()

    def finish_sent(i):
        finish(i)
        v_peer(i).start()
        ship(i)

    def finish_kept(i):
        finish(i)
        ship(i)

    def finish_extra(i):
        wait_y(0, i)
        finish(i)
        ship(i)

    loop(extra, nq, finish_sent)
    loop(nq + early, held, take_extra)
    loop(0, extra, finish_kept)
    loop(nq + early, held, extra_inner)
    loop(nq, held, finish_extra)

    def columns(i):
        return halves(sb[:, place(i, x)])

    def multiply(i):
        v_mate(i).wait_recv()
        part = columns(i)
        for h in range(2):
            pacc[h] += dot3(part, halves(vb[h, chunk(i), :]), NN)

    def multiply_far(i):
        v_peer(i - nq).wait_recv()
        ship(i)
        part = columns(i)
        pacc[k] += dot3(part, halves(vb[k, chunk(i), :]), NN)
        v_mate(i).wait_recv()
        pacc[1 - k] += dot3(part, halves(vb[1 - k, chunk(i), :]), NN)

    loop(0, held, multiply)
    loop(held, 2 * nq, multiply_far)

    for h in range(2):
        for side in range(2):
            pt[h + 2 * side] = pacc[h, :, side * bw : (side + 1) * bw].T

    share = out_ref.shape[0]

    def drain(i):
        x_peer(i).wait_send()
        for p in range(2):
            y_peer(p, i).wait_send()
            y_mate(p, i).wait_send()
            y_forward(p, i).wait_send()

    def drain_v(i):
        v_mate(i).wait_send()
        v_out(i).wait()

    def drain_all():
        for copy in sent:
            copy.wait_send()
        loop(0, held, drain)
        loop(extra, nq, lambda i: v_peer(i).wait_send())
        loop(0, 2 * nq, drain_v)

    total, last = sum_rows(2, lambda zz, yy: pt.at[zz, aligned(yy, share)], pyb, pzb, drain_all)
    out_ref[...] = total
    for copy in last:
        copy.wait_send()


CHUNK = 512
AHEAD = 3
EARLY, LATE = 1, 1


def on_grid(nrow, ncol, eigvecs, reflectors, factors, slab):
    size, bw = eigvecs.shape
    panel = factors.shape[1]
    nz = nrow // 2
    half = size // 2
    q = min(CHUNK, half)
    nq = half // q
    early, late = min(EARLY, nq), min(LATE, nq - min(EARLY, nq))
    extra = early + late
    held = nq + extra
    kept = held * q
    wide = 2 * bw
    f32 = jnp.float32
    rows = wide // nrow
    mine = slab.shape[0]
    share = ncol * bw // nrow
    sem = pltpu.SemaphoreType.DMA
    vmem = pltpu.VMEM
    vectors, product = pl.pallas_call(
        functools.partial(whole_kernel, (nz, q, nq, min(AHEAD, nq), early, late)),
        out_shape=(
            jax.ShapeDtypeStruct((size, bw), f32),
            jax.ShapeDtypeStruct((share, mine), f32),
        ),
        in_specs=[pl.BlockSpec(memory_space=pl.ANY)] * 4,
        out_specs=(pl.BlockSpec(memory_space=pl.ANY), pl.BlockSpec(memory_space=pltpu.VMEM)),
        scratch_shapes=[
            vmem((kept, wide), f32), vmem((kept, panel), f32), vmem((kept, panel), f32),
            vmem(slab.shape, f32), vmem(factors.shape, f32), vmem((2, size, wide), f32),
            vmem((2, wide, panel), f32), vmem((panel, panel), f32), vmem((2, wide, panel), f32), vmem((2, panel, wide), f32),
            vmem((2, nz, rows, panel), f32), vmem((2, nz, rows, panel), f32),
            vmem((2, rows, panel), f32), vmem((2, rows, panel), f32),
            vmem((2, mine, wide), f32), vmem((nz, bw, mine), f32),
            vmem((nz, share, mine), f32), vmem((nz, share, mine), f32),
            sem((held,)), sem((2, held)), sem((2,)),
            sem((held,)), sem((held,)), sem((2, held)), sem((2, held)),
            sem((2, held)), sem((2, held)), sem((2, held)), sem((2, held)),
            sem((3, nz)), sem((3, nz)), sem((3, nz)), sem((3, nz)),
            sem((2,)), sem((2,)),
            sem((2, nz)), sem((2, nz)), sem((2, nz)), sem((2, nz)),
            sem((nq,)), sem((nq,)), sem((2 * nq,)), sem((2 * nq,)), sem((2 * nq,)),
        ],
        compiler_params=pltpu.CompilerParams(
            collective_id=0, has_side_effects=True, vmem_limit_bytes=66_000_000),
        name="whole",
    )(eigvecs, reflectors, factors, slab)
    return vectors, product.T


def on_any(nrow, ncol, eigvecs, reflectors, factors, slab):
    c = lax.axis_index("col")
    first_own, second_own = reflectors[0], reflectors[1]
    all_x, second_y, first_y = (
        lax.all_gather(block, "col", axis=1, tiled=True) for block in (eigvecs, second_own, first_own)
    )
    own = second_own.shape[1]
    both = jnp.concatenate([second_own, first_own], axis=1)
    stacked = jnp.concatenate([tdot(both, all_x), tdot(first_own, second_y)])
    slab_x, slab_second, slab_first = (dot(block, slab, ((0,), (1,))) for block in (all_x, second_y, first_y))
    sums = lax.all_gather(lax.psum(stacked, "row"), "col")
    panel = factors.shape[1]
    second_w, first_raw, gram = (sums[:, i * own : (i + 1) * own].reshape(panel, -1) for i in range(3))
    second_tw = dot(factors[1], second_w)
    first_tw = dot(factors[0], first_raw - dot(gram, second_tw))
    partial = slab_x - tdot(second_tw, slab_second) - tdot(first_tw, slab_first)
    product = lax.psum_scatter(partial, "row", tiled=True)
    vectors = eigvecs
    for block, tw in ((second_y, second_tw), (first_y, first_tw)):
        width = eigvecs.shape[1]
        vectors = vectors - dot(block, lax.dynamic_slice_in_dim(tw, c * width, width, axis=1))
    return vectors, product.T


def solution(mesh):
    nrow, ncol = mesh.shape["row"], mesh.shape["col"]
    fits = ncol == 4 and nrow == 2 * ncol
    return jax.shard_map(
        functools.partial(on_grid if fits else on_any, nrow, ncol),
        mesh=mesh,
        in_specs=(P("row", "col"), P(None, "row", "col"), P(), P("col", "row")),
        out_specs=(P("row", "col"), P("col", "row")),
        check_vma=False,
    )
```

```python
import functools

import jax
import jax.numpy as jnp
from jax import lax
from jax.experimental import pallas as pl
from jax.experimental.pallas import tpu as pltpu
from jax.sharding import PartitionSpec as P

MESH = pl.DeviceIdType.MESH
NN = ((1,), (0,))
NT = ((1,), (1,))
TN = ((0,), (0,))


def dot(left, right, dims=NN):
    return lax.dot_general(
        left, right, (dims, ((), ())), precision=lax.Precision.HIGH, preferred_element_type=jnp.float32
    )


def tdot(left, right):
    return dot(left, right, TN)


def halves(a):
    high = a.astype(jnp.bfloat16)
    return high, (a - high.astype(jnp.float32)).astype(jnp.bfloat16)


def dot3(left, right, dims):
    def one(a, b):
        return lax.dot_general(a, b, (dims, ((), ())), preferred_element_type=jnp.float32)

    (lh, ll), (rh, rl) = left, right
    return one(lh, rh) + (one(lh, rl) + one(ll, rh))


def loop(lo, hi, body):
    if hi - lo == 1:
        body(lo)
    elif hi > lo:
        lax.fori_loop(lo, hi, lambda i, carry: (body(i), carry)[1], 0)


def aligned(i, size):
    return pl.ds(pl.multiple_of(i * size, size), size)


def whole_kernel(
    dims, x_hbm, y_hbm, t_hbm, s_hbm, vec_hbm, out_ref,
    xb, xt, y1b, y2b, sb, tb, vt, vst, w, gram, wf, tw, ybuf, zbuf, xs, xr, pt, pyb, pzb,
    lx, ly, ls, px_s, px_r, py_s, py_r, m_s, m_r, f_s, f_r,
    ry_s, ry_r, rz_s, rz_r, rx_s, rx_r, gz_s, gz_r, gy_s, gy_r,
    vp_s, vp_r, vm_s, vm_r, vo,
):
    nz, q, nq, ahead, early, late = dims
    groups = pt.shape[0]
    extra = early + late
    held = nq + extra
    bw = x_hbm.shape[1]
    share = out_ref.shape[0]
    part = share // groups
    span = xt.shape[0] // groups
    r, c = lax.axis_index("row"), lax.axis_index("col")
    z, y = r // 2, lax.rem(r, 2)
    x, k = c // 2, lax.rem(c, 2)
    mate = (r, c + 1 - 2 * k)
    peer = (r, c + 2 - 4 * x)
    peer_block = c + 2 - 4 * x
    ynext = (r + 1 - 2 * y, c)

    def zat(d):
        return lax.rem(z + d, nz)

    def znext(d):
        return (zat(d) * 2 + y, c)

    partners = [mate, peer, ynext] + [znext(d) for d in range(1, nz)]
    barrier = pltpu.get_barrier_semaphore()
    for other in partners:
        pl.semaphore_signal(barrier, inc=1, device_id=other, device_id_type=MESH)
    pl.semaphore_wait(barrier, len(partners))

    def send(src, dst, s, t, device):
        return pltpu.make_async_remote_copy(src, dst, s, t, device_id=device, device_id_type=MESH)

    def chunk(i):
        return aligned(i, q)

    def place(i, side):
        within = lax.rem(i, nq)
        half = jnp.where(i < nq, side, 1 - side)
        return pl.ds(pl.multiple_of((half * nq + within) * q, q), q)

    def lanes(b):
        return aligned(b, bw)

    panels = (y1b, y2b)

    def x_local(i):
        return pltpu.make_async_copy(x_hbm.at[place(i, x)], xb.at[chunk(i), lanes(x)], lx.at[i])

    def x_peer(i):
        return send(x_hbm.at[place(i, 1 - x)], xb.at[chunk(i), lanes(x)], px_s.at[i], px_r.at[i], peer)

    def y_local(p, i):
        return pltpu.make_async_copy(y_hbm.at[p, place(i, x)], panels[p].at[chunk(i), lanes(c)], ly.at[p, i])

    def y_peer(p, i):
        return send(
            y_hbm.at[p, place(i, 1 - x)], panels[p].at[chunk(i), lanes(c)], py_s.at[p, i], py_r.at[p, i], peer)

    def y_mate(p, i):
        return send(y_hbm.at[p, place(i, x)], panels[p].at[chunk(i), lanes(c)], m_s.at[p, i], m_r.at[p, i], mate)

    def y_forward(p, i):
        block = panels[p].at[chunk(i), lanes(peer_block)]
        return send(block, block, f_s.at[p, i], f_r.at[p, i], mate)

    def wait_y(p, i):
        y_local(p, i).wait()
        y_mate(p, i).wait_recv()
        y_forward(p, i).wait_recv()

    def pass_on(p, i):
        y_peer(p, i).wait_recv()
        y_forward(p, i).start()

    def send_bulk(i):
        x_peer(i).start()
        y_peer(1, i).start()
        y_peer(0, i).start()

    def first_two(i):
        x_peer(i).start()
        y_peer(1, i).start()

    loop(0, nq, first_two)
    loop(0, ahead, lambda i: y_peer(0, i).start())

    def own(i):
        x_local(i).start()
        y_mate(1, i).start()
        y_local(1, i).start()
        y_mate(0, i).start()
        y_local(0, i).start()

    loop(0, held, own)
    t_copy = pltpu.make_async_copy(t_hbm, tb, ls.at[0])
    s_copy = pltpu.make_async_copy(s_hbm, sb, ls.at[1])
    t_copy.start()
    s_copy.start()

    w[...] = jnp.zeros_like(w)
    gram[...] = jnp.zeros_like(gram)
    pt[...] = jnp.zeros_like(pt)

    def pieces(block, side):
        for g in range(groups):
            for half in range(bw // share):
                yield block + half * share + g * part, g * span + (side * (bw // share) + half) * part

    def turn(i):
        x_local(i).wait()
        x_peer(i).wait_recv()
        turned = xb[chunk(i), :].T
        for side in range(2):
            for src, dst in pieces(side * bw, side):
                xt[dst : dst + part, chunk(i)] = turned[src : src + part]

    def step(i):
        @pl.when(i < nq)
        def _():
            pass_on(1, i)

        @pl.when(i > 0)
        def _():
            j = i - 1
            turn(j)
            wait_y(1, j)
            w[0] += dot3(halves(xt[:, chunk(j)]), halves(y2b[chunk(j), :]), NN)

    loop(0, nq + 1, step)
    t_copy.wait()
    s_copy.wait()

    rows = w.shape[1] // (2 * nz)

    class Sum:
        def __init__(self, n, piece, ys, zs):
            self.order = list(range(1, nz)) + [0]
            self.piece, self.zs, self.ys = piece, zs, ys
            self.out = [
                send(piece(zat(d), 1 - y), ys.at[d], ry_s.at[n, d], ry_r.at[n, d], ynext) for d in self.order]
            self.hops = [send(piece(zat(d), y), zs.at[d], rz_s.at[n, d], rz_r.at[n, d], znext(d)) for d in range(1, nz)]
            for copy in self.out:
                copy.start()

        def relay(self):
            for d, copy in zip(self.order, self.out):
                copy.wait_recv()
                if d:
                    self.piece(zat(d), y)[...] += self.ys[d]
                    self.hops[d - 1].start()

        def total(self):
            total = self.piece(z, y)[...] + self.ys[0]
            for d in range(1, nz):
                self.hops[d - 1].wait_recv()
                total = total + self.zs[d]
            return total

        def wait_sends(self):
            for copy in self.out + self.hops:
                copy.wait_send()

    def all_sum(n, meanwhile, after_exchange, after_sends, before_last):
        def piece(zz, yy):
            return w.at[n, aligned(zz * 2 + yy, rows)]

        def final(zz, yy):
            return wf.at[n, aligned(zz * 2 + yy, rows)]

        reduced = Sum(n, piece, ybuf.at[n], zbuf.at[n])
        reduced.relay()
        meanwhile()
        xs[n] = reduced.total()
        swap = send(xs.at[n], xr.at[n], rx_s.at[n], rx_r.at[n], peer)
        swap.start()
        after_exchange()
        swap.wait_recv()
        mine = final(z, y)
        mine[...] = xs[n] + xr[n]
        along = [send(mine, mine, gz_s.at[n, d], gz_r.at[n, d], znext(d)) for d in range(1, nz)]
        for copy in along:
            copy.start()
        across = [send(mine, mine, gy_s.at[n, 0], gy_r.at[n, 0], ynext)]
        across[0].start()
        after_sends()
        for d in range(1, nz):
            along[d - 1].wait_recv()
            block = final(lax.rem(z + nz - d, nz), y)
            across.append(send(block, block, gy_s.at[n, d], gy_r.at[n, d], ynext))
            across[-1].start()
        before_last()
        for copy in across:
            copy.wait_recv()
        return reduced.out + reduced.hops + [swap] + along + across

    def inner(i):
        xt[:, chunk(i)] = xt[:, chunk(i)] - dot3(halves(tw[1]), halves(y2b[chunk(i), :]), NT)

    def apply(p, n):
        tw[p] = dot3(halves(wf[n]), halves(tb[p]), NT)

    def raw(i):
        wait_y(0, i)
        first = halves(y1b[chunk(i), :])
        w[1] += dot3(halves(xt[:, chunk(i)]), first, NN)
        gram[...] += dot3(halves(y2b[chunk(i), :]), first, TN)

    def rest():
        loop(ahead, nq, lambda i: y_peer(0, i).start())
        loop(nq, nq + early, send_bulk)
        loop(0, nq - 2, lambda i: pass_on(0, i))
        loop(0, nq - 2, raw)

    def nearly():
        pass_on(0, nq - 2)
        raw(nq - 2)

    sent = all_sum(0, lambda: None, rest, nearly, lambda: pass_on(0, nq - 1))
    apply(1, 0)
    raw(nq - 1)
    w[1] = w[1] - dot3(halves(tw[1]), halves(gram[...]), NN)

    def take_extra(i):
        pass_on(1, i)
        pass_on(0, i)

    def extra_inner(i):
        turn(i)
        wait_y(1, i)
        inner(i)

    def early_extra():
        loop(nq, nq + early, take_extra)
        loop(nq, nq + early, extra_inner)

    sent += all_sum(
        1, lambda: loop(0, nq, inner), lambda: loop(nq + early, held, send_bulk), lambda: None, early_extra)
    apply(0, 1)

    def columns(g):
        return pl.ds(g * span, span)

    def v_mate(g, i):
        block = vt.at[k, columns(g), chunk(i)]
        return send(block, block, vm_s.at[g, i], vm_r.at[g, i], mate)

    def v_peer(g, i):
        return send(
            vt.at[k, columns(g), chunk(i)], vt.at[k, columns(g), chunk(i + nq)], vp_s.at[g, i], vp_r.at[g, i], peer)

    def v_out(i):
        return pltpu.make_async_copy(vst.at[chunk(i)], vec_hbm.at[place(i, x)], vo.at[i])

    def write_out(i):
        for side in range(2):
            @pl.when(x == side)
            def _():
                block = [None] * (bw // part)
                for src, dst in pieces(0, side):
                    block[src // part] = vt[k, dst : dst + part, chunk(i)]
                vst[chunk(i), :] = jnp.concatenate(block, axis=0).T
        v_out(i).start()

    def finish(i):
        vt[k, :, chunk(i)] = xt[:, chunk(i)] - dot3(halves(tw[0]), halves(y1b[chunk(i), :]), NT)

    def ship(i):
        for g in range(groups):
            v_mate(g, i).start()

    def finish_sent(i):
        finish(i)
        v_peer(0, i).start()
        ship(i)

    def finish_kept(i):
        finish(i)
        ship(i)

    def finish_extra(i):
        wait_y(0, i)
        finish(i)
        ship(i)

    loop(extra, nq, finish_sent)
    for g in range(1, groups):
        loop(extra, nq, lambda i: v_peer(g, i).start())
    loop(nq + early, held, take_extra)
    loop(0, extra, finish_kept)
    loop(nq + early, held, extra_inner)
    loop(nq, held, finish_extra)

    def multiply(i):
        for g in range(groups):
            v_mate(g, i).wait_recv()
        right = halves(sb[:, place(i, x)])
        for h in range(2):
            added = dot3(halves(vt[h, :, chunk(i)]), right, NT)
            for g in range(groups):
                pt[g, h] += added[g * span : (g + 1) * span]

    def multiply_far(g, i):
        v_peer(g, i - nq).wait_recv()
        v_mate(g, i).start()
        right = halves(sb[:, place(i, x)])
        pt[g, k] += dot3(halves(vt[k, columns(g), chunk(i)]), right, NT)
        v_mate(g, i).wait_recv()
        pt[g, 1 - k] += dot3(halves(vt[1 - k, columns(g), chunk(i)]), right, NT)

    def scatter(g):
        def piece(zz, yy):
            return pt.at[g, lax.rem(zz, 2), aligned((zz // 2) * 2 + yy, part)]

        return Sum(2 + g, piece, pyb.at[g], pzb.at[g])

    def collect(g):
        out_ref[g * part : (g + 1) * part, :] = last[g].total()

    loop(0, held, multiply)
    loop(0, held, write_out)
    last = []
    for g in range(groups):
        for i in range(held, 2 * nq):
            multiply_far(g, i)
            if g and i == held:
                last[g - 1].relay()
        if g and held == 2 * nq:
            last[g - 1].relay()
        last.append(scatter(g))
        if g:
            collect(g - 1)

    def drain(i):
        x_peer(i).wait_send()
        for p in range(2):
            y_peer(p, i).wait_send()
            y_mate(p, i).wait_send()
            y_forward(p, i).wait_send()

    def drain_v(i):
        for g in range(groups):
            v_mate(g, i).wait_send()
        v_out(i).wait()

    last[-1].relay()
    loop(held, 2 * nq, write_out)
    for copy in sent:
        copy.wait_send()
    loop(0, held, drain)
    for g in range(groups):
        loop(extra, nq, lambda i: v_peer(g, i).wait_send())
    loop(0, 2 * nq, drain_v)
    collect(groups - 1)
    for done in last:
        done.wait_sends()


CHUNK = 512
GROUPS = 2
AHEAD = 3
EARLY, LATE = 1, 1


def on_grid(nrow, ncol, eigvecs, reflectors, factors, slab):
    size, bw = eigvecs.shape
    panel = factors.shape[1]
    nz = nrow // 2
    half = size // 2
    q = min(CHUNK, half)
    nq = half // q
    early, late = min(EARLY, nq), min(LATE, nq - min(EARLY, nq))
    held = nq + early + late
    kept = held * q
    wide = 2 * bw
    f32 = jnp.float32
    rows = wide // nrow
    mine = slab.shape[0]
    share = ncol * bw // nrow
    g = GROUPS
    part = share // g
    sem = pltpu.SemaphoreType.DMA
    vmem = pltpu.VMEM
    vectors, product = pl.pallas_call(
        functools.partial(whole_kernel, (nz, q, nq, min(AHEAD, nq), early, late)),
        out_shape=(
            jax.ShapeDtypeStruct((size, bw), f32),
            jax.ShapeDtypeStruct((share, mine), f32),
        ),
        in_specs=[pl.BlockSpec(memory_space=pltpu.HBM)] * 4,
        out_specs=(pl.BlockSpec(memory_space=pl.ANY), pl.BlockSpec(memory_space=pltpu.VMEM)),
        scratch_shapes=[
            vmem((kept, wide), f32), vmem((wide, kept), f32), vmem((kept, panel), f32), vmem((kept, panel), f32),
            vmem(slab.shape, f32), vmem(factors.shape, f32), vmem((2, wide, size), f32), vmem((size, bw), f32),
            vmem((2, wide, panel), f32), vmem((panel, panel), f32),
            vmem((2, wide, panel), f32), vmem((2, wide, panel), f32),
            vmem((2, nz, rows, panel), f32), vmem((2, nz, rows, panel), f32),
            vmem((2, rows, panel), f32), vmem((2, rows, panel), f32),
            vmem((g, 2, wide // g, mine), f32),
            vmem((g, nz, part, mine), f32), vmem((g, nz, part, mine), f32),
            sem((held,)), sem((2, held)), sem((2,)),
            sem((held,)), sem((held,)), sem((2, held)), sem((2, held)),
            sem((2, held)), sem((2, held)), sem((2, held)), sem((2, held)),
            sem((2 + g, nz)), sem((2 + g, nz)), sem((2 + g, nz)), sem((2 + g, nz)),
            sem((2,)), sem((2,)),
            sem((2, nz)), sem((2, nz)), sem((2, nz)), sem((2, nz)),
            sem((g, nq)), sem((g, nq)), sem((g, 2 * nq)), sem((g, 2 * nq)), sem((2 * nq,)),
        ],
        compiler_params=pltpu.CompilerParams(
            collective_id=0, has_side_effects=True, vmem_limit_bytes=VMEM_BYTES),
        name="whole",
    )(eigvecs, reflectors, factors, slab)
    return vectors, product.T


VMEM_BYTES = 52_000_000


def on_any(nrow, ncol, eigvecs, reflectors, factors, slab):
    c = lax.axis_index("col")
    first_own, second_own = reflectors[0], reflectors[1]
    all_x, second_y, first_y = (
        lax.all_gather(block, "col", axis=1, tiled=True) for block in (eigvecs, second_own, first_own)
    )
    own = second_own.shape[1]
    both = jnp.concatenate([second_own, first_own], axis=1)
    stacked = jnp.concatenate([tdot(both, all_x), tdot(first_own, second_y)])
    slab_x, slab_second, slab_first = (dot(block, slab, ((0,), (1,))) for block in (all_x, second_y, first_y))
    sums = lax.all_gather(lax.psum(stacked, "row"), "col")
    panel = factors.shape[1]
    second_w, first_raw, gram = (sums[:, i * own : (i + 1) * own].reshape(panel, -1) for i in range(3))
    second_tw = dot(factors[1], second_w)
    first_tw = dot(factors[0], first_raw - dot(gram, second_tw))
    partial = slab_x - tdot(second_tw, slab_second) - tdot(first_tw, slab_first)
    product = lax.psum_scatter(partial, "row", tiled=True)
    vectors = eigvecs
    for block, tw in ((second_y, second_tw), (first_y, first_tw)):
        width = eigvecs.shape[1]
        vectors = vectors - dot(block, lax.dynamic_slice_in_dim(tw, c * width, width, axis=1))
    return vectors, product.T


def solution(mesh):
    nrow, ncol = mesh.shape["row"], mesh.shape["col"]
    fits = ncol == 4 and nrow == 2 * ncol
    return jax.shard_map(
        functools.partial(on_grid if fits else on_any, nrow, ncol),
        mesh=mesh,
        in_specs=(P("row", "col"), P(None, "row", "col"), P(), P("col", "row")),
        out_specs=(P("row", "col"), P("col", "row")),
        check_vma=False,
    )
```

```python
import functools

import jax
import jax.numpy as jnp
from jax import lax
from jax.experimental import pallas as pl
from jax.experimental.pallas import tpu as pltpu
from jax.sharding import PartitionSpec as P

MESH = pl.DeviceIdType.MESH
NN = ((1,), (0,))
NT = ((1,), (1,))
TN = ((0,), (0,))


def dot(left, right, dims=NN):
    return lax.dot_general(
        left, right, (dims, ((), ())), precision=lax.Precision.HIGH, preferred_element_type=jnp.float32
    )


def tdot(left, right):
    return dot(left, right, TN)


def halves(a):
    high = a.astype(jnp.bfloat16)
    return high, (a - high.astype(jnp.float32)).astype(jnp.bfloat16)


def dot3(left, right, dims):
    def one(a, b):
        return lax.dot_general(a, b, (dims, ((), ())), preferred_element_type=jnp.float32)

    (lh, ll), (rh, rl) = left, right
    return one(lh, rh) + (one(lh, rl) + one(ll, rh))


def whole_kernel(
    plan, x_hbm, y_hbm, t_hbm, s_hbm, vec_hbm, out_ref,
    xb, xt, y1b, y2b, sb, far_h, far_l, tb, vt, vst, w, gram, wf, tw, ybuf, zbuf, xs, xr, pt, pyb, pzb,
    ls, bulk_s, x_r, y_r, py_r, ry_r, rz_r, r_s, rx_s, rx_r, gz_r, gy_r, g_s, vp_r, vm_r, v_s,
):
    nz, q, nq, ahead, early, late, kept, sent, parts = plan
    half = nq * q
    must = [(i * q, q) for i in range(nq)]
    extras = early + late
    held = half + sum(n for _, n in extras)
    bw = x_hbm.shape[1]
    share = out_ref.shape[0]
    per = bw // share
    offs = [sum(parts[:g]) for g in range(len(parts))]
    spans = [(2 * per * o, 2 * per * n) for o, n in zip(offs, parts)]
    first_span = spans[0][1]
    wide = xt.shape[0]
    r, c = lax.axis_index("row"), lax.axis_index("col")
    z, y = r // 2, lax.rem(r, 2)
    x, k = c // 2, lax.rem(c, 2)
    mate = (r, c + 1 - 2 * k)
    peer = (r, c + 2 - 4 * x)
    peer_block = c + 2 - 4 * x
    ynext = (r + 1 - 2 * y, c)

    def zat(d):
        return lax.rem(z + d, nz)

    def znext(d):
        return (zat(d) * 2 + y, c)

    partners = [mate, peer, ynext] + [znext(d) for d in range(1, nz)]
    barrier = pltpu.get_barrier_semaphore()
    for other in partners:
        pl.semaphore_signal(barrier, inc=1, device_id=other, device_id_type=MESH)
    pl.semaphore_wait(barrier, len(partners))

    def send(src, dst, s, t, device):
        return pltpu.make_async_remote_copy(src, dst, s, t, device_id=device, device_id_type=MESH)

    def sent_all(ref, s):
        send(ref, ref, s, s, mate).wait_send()

    def at(m):
        return pl.ds(m[0], m[1])

    def place(m, side):
        start, size = m
        base = side * half + start if start < half else (1 - side) * half + start - half
        return pl.ds(pl.multiple_of(base, 128), size)

    def lanes(b):
        return pl.ds(pl.multiple_of(b * bw, bw), bw)

    def index(m):
        return m[0] // q if m[0] < half else nq + extras.index(m)

    panels = (y1b, y2b)

    def x_local(m):
        return pltpu.make_async_copy(x_hbm.at[place(m, x)], xb.at[at(m), lanes(x)], x_r.at[index(m)])

    def x_peer(m):
        return send(x_hbm.at[place(m, 1 - x)], xb.at[at(m), lanes(x)], bulk_s.at[0], x_r.at[index(m)], peer)

    def y_local(p, m):
        return pltpu.make_async_copy(
            y_hbm.at[p, place(m, x)], panels[p].at[at(m), lanes(c)], y_r.at[p, index(m)])

    def y_peer(p, m):
        return send(
            y_hbm.at[p, place(m, 1 - x)], panels[p].at[at(m), lanes(c)], bulk_s.at[1], py_r.at[p, index(m)], peer)

    def y_mate(p, m):
        return send(
            y_hbm.at[p, place(m, x)], panels[p].at[at(m), lanes(c)], bulk_s.at[2], y_r.at[p, index(m)], mate)

    def y_forward(p, m):
        block = panels[p].at[at(m), lanes(peer_block)]
        return send(block, block, bulk_s.at[3], y_r.at[p, index(m)], mate)

    def wait_y(p, m):
        block = panels[p].at[at(m), pl.ds(0, 3 * bw)]
        pltpu.make_async_copy(block, block, y_r.at[p, index(m)]).wait()

    def pass_on(p, m):
        y_peer(p, m).wait_recv()
        y_forward(p, m).start()

    def send_bulk(m):
        x_peer(m).start()
        y_peer(1, m).start()
        y_peer(0, m).start()

    for m in must:
        x_peer(m).start()
        y_peer(1, m).start()
    for m in must[:ahead]:
        y_peer(0, m).start()
    for m in must + extras:
        x_local(m).start()
        for p in (1, 0):
            y_mate(p, m).start()
            y_local(p, m).start()
    t_copy = pltpu.make_async_copy(t_hbm, tb, ls.at[0])
    s_copy = pltpu.make_async_copy(s_hbm, sb, ls.at[1])
    t_copy.start()
    s_copy.start()

    w[...] = jnp.zeros_like(w)
    gram[...] = jnp.zeros_like(gram)
    pt[...] = jnp.zeros_like(pt)
    t_copy.wait()
    s_copy.wait()
    far = [(start + half, size) for start, size in sent]
    reach = far[0][0]
    for m in far:
        high, low = halves(sb[:, place(m, x)])
        far_h[:, m[0] - reach : m[0] - reach + m[1]] = high
        far_l[:, m[0] - reach : m[0] - reach + m[1]] = low

    def pieces(block, side):
        for o, n, (base, _) in zip(offs, parts, spans):
            for h in range(per):
                yield block + h * share + o, base + (side * per + h) * n, n

    def turn(m):
        pltpu.make_async_copy(xb.at[at(m)], xb.at[at(m)], x_r.at[index(m)]).wait()
        turned = xb[at(m), :].T
        for side in range(2):
            for src, dst, n in pieces(side * bw, side):
                xt[dst : dst + n, at(m)] = turned[src : src + n]

    def begin(m):
        turn(m)
        wait_y(1, m)
        w[0] += dot3(halves(xt[:, at(m)]), halves(y2b[at(m), :]), NN)

    for i, m in enumerate(must):
        pass_on(1, m)
        if i:
            begin(must[i - 1])
    begin(must[-1])

    class Sum:
        def __init__(self, n, piece, ys, zs, whole):
            self.n, self.piece, self.ys, self.zs, self.whole = n, piece, ys, zs, whole
            self.order = list(range(1, nz)) + [0]
            self.out = [
                send(piece(zat(d), 1 - y), ys(d), r_s.at[n], ry_r.at[n, d], ynext) for d in self.order]
            self.hops = [send(piece(zat(d), y), zs(d), r_s.at[n], rz_r.at[n, d], znext(d)) for d in range(1, nz)]
            for copy in self.out:
                copy.start()

        def relay(self):
            for d, copy in zip(self.order, self.out):
                copy.wait_recv()
                if d:
                    self.piece(zat(d), y)[...] += self.ys(d)[...]
                    self.hops[d - 1].start()

        def total(self):
            total = self.piece(z, y)[...] + self.ys(0)[...]
            for d in range(1, nz):
                self.hops[d - 1].wait_recv()
                total = total + self.zs(d)[...]
            return total

        def drain(self):
            sent_all(self.whole, r_s.at[self.n])

    class AllSum:
        def __init__(self, n, panel, base, size):
            self.n = n
            rows = size // (2 * nz)
            self.rows = pl.ds(base // (2 * nz), rows)

            def block(ref, zz, yy):
                return ref.at[panel, pl.ds(pl.multiple_of(base + (zz * 2 + yy) * rows, 8), rows)]

            self.final = lambda zz, yy: block(wf, zz, yy)
            self.whole = w.at[panel, pl.ds(0, (2 * nz - 1) * rows)]
            self.panel = panel
            self.sum = Sum(
                n, lambda zz, yy: block(w, zz, yy),
                lambda d: ybuf.at[panel, d, self.rows], lambda d: zbuf.at[panel, d, self.rows], self.whole)
            self.relay = self.sum.relay

        def swap(self):
            n = self.n
            mine, other = xs.at[self.panel, self.rows], xr.at[self.panel, self.rows]
            mine[...] = self.sum.total()
            self.swapped = send(mine, other, rx_s.at[n], rx_r.at[n], peer)
            self.swapped.start()

        def gather(self):
            n = self.n
            self.swapped.wait_recv()
            mine = self.final(z, y)
            mine[...] = xs[self.panel, self.rows] + xr[self.panel, self.rows]
            self.along = [send(mine, mine, g_s.at[n], gz_r.at[n, d], znext(d)) for d in range(1, nz)]
            for copy in self.along:
                copy.start()
            self.across = [send(mine, mine, g_s.at[n], gy_r.at[n, 0], ynext)]
            self.across[0].start()

        def forward(self):
            for d in range(1, nz):
                self.along[d - 1].wait_recv()
                block = self.final(lax.rem(z + nz - d, nz), y)
                self.across.append(send(block, block, g_s.at[self.n], gy_r.at[self.n, d], ynext))
                self.across[-1].start()

        def finish(self):
            for copy in self.across:
                copy.wait_recv()

        def drain(self):
            self.sum.drain()
            self.swapped.wait_send()
            sent_all(self.whole, g_s.at[self.n])

    def inner(m):
        xt[:, at(m)] = xt[:, at(m)] - dot3(halves(tw[1]), halves(y2b[at(m), :]), NT)

    def raw(m):
        wait_y(0, m)
        first = halves(y1b[at(m), :])
        w[1] += dot3(halves(xt[:, at(m)]), first, NN)
        gram[...] += dot3(halves(y2b[at(m), :]), first, TN)

    a0 = AllSum(0, 0, 0, wide)
    a0.relay()
    a0.swap()
    for m in must[ahead:]:
        y_peer(0, m).start()
    for m in early:
        send_bulk(m)
    for m in must[:-2]:
        pass_on(0, m)
    for m in must[:-2]:
        raw(m)
    a0.gather()
    pass_on(0, must[-2])
    raw(must[-2])
    a0.forward()
    pass_on(0, must[-1])
    a0.finish()
    tw[1] = dot3(halves(wf[0]), halves(tb[1]), NT)
    raw(must[-1])
    w[1] = w[1] - dot3(halves(tw[1]), halves(gram[...]), NN)

    def take(m):
        pass_on(1, m)
        pass_on(0, m)

    def extra_inner(m):
        turn(m)
        wait_y(1, m)
        inner(m)

    a1 = AllSum(1, 1, 0, first_span)
    a2 = AllSum(2, 1, first_span, wide - first_span)
    a1.relay()
    a2.relay()
    for m in must:
        inner(m)
    a1.swap()
    a2.swap()
    for m in late:
        send_bulk(m)
    a1.gather()
    a2.gather()
    a1.forward()
    a2.forward()
    for m in early:
        take(m)
    for m in early:
        extra_inner(m)

    def band(g):
        return pl.ds(*spans[g])

    later = pl.ds(first_span, wide - first_span)
    locals_ = sent + kept + extras

    def v_mate(b, rows, m):
        block = vt.at[k, rows, at(m)]
        slot = locals_.index(m) if m in locals_ else len(locals_) + far.index(m)
        return send(block, block, v_s.at[1], vm_r.at[b, slot], mate)

    def v_peer(g, j):
        return send(vt.at[k, band(g), at(sent[j])], vt.at[k, band(g), at(far[j])], v_s.at[0], vp_r.at[g, j], peer)

    def v_out(m):
        return pltpu.make_async_copy(vst.at[at(m)], vec_hbm.at[place(m, x)], v_s.at[2])

    def write_out(m):
        for side in range(2):
            @pl.when(x == side)
            def _():
                block = [vt[k, dst : dst + n, at(m)] for _, dst, n in sorted(pieces(0, side))]
                vst[at(m), :] = jnp.concatenate(block, axis=0).T
        v_out(m).start()

    def weigh(rows):
        tw[0, rows, :] = dot3(halves(wf[1, rows, :]), halves(tb[0]), NT)

    def finish(rows, m):
        vt[k, rows, at(m)] = xt[rows, at(m)] - dot3(halves(tw[0, rows, :]), halves(y1b[at(m), :]), NT)

    a1.finish()
    weigh(band(0))
    for j, m in enumerate(sent):
        finish(band(0), m)
        v_peer(0, j).start()
    a2.finish()
    weigh(later)
    for j, m in enumerate(sent):
        finish(later, m)
        v_peer(1, j).start()
    for g in range(2, len(parts)):
        for j in range(len(sent)):
            v_peer(g, j).start()
    everything = pl.ds(0, wide)
    for m in sent:
        v_mate(0, everything, m).start()
    for m in kept:
        finish(everything, m)
        v_mate(0, everything, m).start()
    for m in late:
        take(m)
    for m in early:
        wait_y(0, m)
        finish(everything, m)
        v_mate(0, everything, m).start()

    def multiply(m):
        v_mate(0, everything, m).wait_recv()
        right = halves(sb[:, place(m, x)])
        for h in range(2):
            pt[h] += dot3(halves(vt[h, :, at(m)]), right, NT)

    for m in sent + kept:
        multiply(m)
    for m in late:
        extra_inner(m)
        wait_y(0, m)
        finish(everything, m)
        v_mate(0, everything, m).start()
    for m in extras:
        multiply(m)
    for m in locals_:
        write_out(m)

    def multiply_far(g, j, h):
        m = far[j]
        cut = slice(m[0] - reach, m[0] - reach + m[1])
        right = far_h[:, cut], far_l[:, cut]
        pt[h, band(g), :] += dot3(halves(vt[h, band(g), at(m)]), right, NT)

    def scatter(g):
        n = parts[g]

        def piece(zz, yy):
            start = spans[g][0] + ((zz // 2) * per + yy) * n
            return pt.at[lax.rem(zz, 2), pl.ds(pl.multiple_of(start, 8), n)]

        def rows(ref):
            return lambda d: ref.at[d, pl.ds(offs[g], n)]

        return Sum(3 + g, piece, rows(pyb), rows(pzb), pt.at[0, pl.ds(0, (2 * nz - 1) * n)])

    def collect(g):
        out_ref[offs[g] : offs[g] + parts[g], :] = last[g].total()

    last = []
    todo = [(g, j) for g in range(len(parts)) for j in range(len(sent))]

    def mate_half(g, j):
        v_mate(g, band(g), far[j]).wait_recv()
        multiply_far(g, j, 1 - k)
        if j == len(sent) - 1:
            last.append(scatter(g))
        elif g and j == 0:
            last[g - 1].relay()

    for t, (g, j) in enumerate(todo):
        v_peer(g, j).wait_recv()
        v_mate(g, band(g), far[j]).start()
        multiply_far(g, j, k)
        if t:
            mate_half(*todo[t - 1])
    mate_half(*todo[-1])
    for g in range(len(parts) - 1):
        collect(g)
    last[-1].relay()
    for m in far:
        write_out(m)
    for s in (a0, a1, a2):
        s.drain()
    sent_all(x_hbm.at[pl.ds(0, held)], bulk_s.at[0])
    for i in (1, 2, 3):
        sent_all(y_hbm.at[:, pl.ds(0, held)], bulk_s.at[i])
    sent_all(vt.at[0, :, pl.ds(0, sum(n for _, n in sent))], v_s.at[0])
    sent_all(vt.at[0], v_s.at[1])
    pltpu.make_async_copy(vst, vec_hbm, v_s.at[2]).wait()
    collect(len(parts) - 1)
    for done in last:
        done.drain()


CHUNK = 4
AHEAD = 3
EARLY = (3,)
LATE = (2,)
PARTS = (4, 2, 2)
UNITS = 16
VMEM_BYTES = 54_000_000


def on_grid(nrow, ncol, eigvecs, reflectors, factors, slab):
    size, bw = eigvecs.shape
    panel = factors.shape[1]
    nz = nrow // 2
    half = size // 2
    unit = half // UNITS
    q = CHUNK * unit
    nq = half // q

    def ranges(start, sizes):
        out = []
        for n in sizes:
            out.append((start, n * unit))
            start += n * unit
        return out

    early = ranges(half, EARLY)
    late = ranges(half + sum(n for _, n in early), LATE)
    extra = sum(EARLY) + sum(LATE)
    kept = ranges(0, (extra,))
    first = (UNITS - extra) % CHUNK
    sent = ranges(extra * unit, ((first,) if first else ()) + (CHUNK,) * ((UNITS - extra) // CHUNK))
    held = half + extra * unit
    away = half - extra * unit
    wide = 2 * bw
    f32 = jnp.float32
    rows = wide // nrow
    mine = slab.shape[0]
    share = ncol * bw // nrow
    parts = tuple(n * share // sum(PARTS) for n in PARTS)
    g = len(parts)
    chunks = nq + len(EARLY) + len(LATE)
    slots = 2 * len(sent) + len(kept) + len(EARLY) + len(LATE)
    sem = pltpu.SemaphoreType.DMA
    vmem = pltpu.VMEM
    vectors, product = pl.pallas_call(
        functools.partial(whole_kernel, (nz, q, nq, AHEAD, early, late, kept, sent, parts)),
        out_shape=(
            jax.ShapeDtypeStruct((size, bw), f32),
            jax.ShapeDtypeStruct((share, mine), f32),
        ),
        in_specs=[pl.BlockSpec(memory_space=pltpu.HBM)] * 4,
        out_specs=(pl.BlockSpec(memory_space=pl.ANY), pl.BlockSpec(memory_space=pltpu.VMEM)),
        scratch_shapes=[
            vmem((held, wide), f32), vmem((wide, held), f32), vmem((held, panel), f32), vmem((held, panel), f32),
            vmem(slab.shape, f32), vmem((mine, away), jnp.bfloat16), vmem((mine, away), jnp.bfloat16),
            vmem(factors.shape, f32), vmem((2, wide, size), f32), vmem((size, bw), f32),
            vmem((2, wide, panel), f32), vmem((panel, panel), f32),
            vmem((2, wide, panel), f32), vmem((2, wide, panel), f32),
            vmem((2, nz, rows, panel), f32), vmem((2, nz, rows, panel), f32),
            vmem((2, rows, panel), f32), vmem((2, rows, panel), f32),
            vmem((2, wide, mine), f32),
            vmem((nz, share, mine), f32), vmem((nz, share, mine), f32),
            sem((2,)), sem((4,)), sem((chunks,)), sem((2, chunks)), sem((2, chunks)),
            sem((3 + g, nz)), sem((3 + g, nz)), sem((3 + g,)), sem((3,)), sem((3,)),
            sem((3, nz)), sem((3, nz)), sem((3,)), sem((g, len(sent))), sem((g, slots)), sem((3,)),
        ],
        compiler_params=pltpu.CompilerParams(
            collective_id=0, has_side_effects=True, vmem_limit_bytes=VMEM_BYTES),
        name="whole",
    )(eigvecs, reflectors, factors, slab)
    return vectors, product.T


def on_any(nrow, ncol, eigvecs, reflectors, factors, slab):
    c = lax.axis_index("col")
    first_own, second_own = reflectors[0], reflectors[1]
    all_x, second_y, first_y = (
        lax.all_gather(block, "col", axis=1, tiled=True) for block in (eigvecs, second_own, first_own)
    )
    own = second_own.shape[1]
    both = jnp.concatenate([second_own, first_own], axis=1)
    stacked = jnp.concatenate([tdot(both, all_x), tdot(first_own, second_y)])
    slab_x, slab_second, slab_first = (dot(block, slab, ((0,), (1,))) for block in (all_x, second_y, first_y))
    sums = lax.all_gather(lax.psum(stacked, "row"), "col")
    panel = factors.shape[1]
    second_w, first_raw, gram = (sums[:, i * own : (i + 1) * own].reshape(panel, -1) for i in range(3))
    second_tw = dot(factors[1], second_w)
    first_tw = dot(factors[0], first_raw - dot(gram, second_tw))
    partial = slab_x - tdot(second_tw, slab_second) - tdot(first_tw, slab_first)
    product = lax.psum_scatter(partial, "row", tiled=True)
    vectors = eigvecs
    for block, tw in ((second_y, second_tw), (first_y, first_tw)):
        width = eigvecs.shape[1]
        vectors = vectors - dot(block, lax.dynamic_slice_in_dim(tw, c * width, width, axis=1))
    return vectors, product.T


def solution(mesh):
    nrow, ncol = mesh.shape["row"], mesh.shape["col"]
    fits = ncol == 4 and nrow == 2 * ncol
    return jax.shard_map(
        functools.partial(on_grid if fits else on_any, nrow, ncol),
        mesh=mesh,
        in_specs=(P("row", "col"), P(None, "row", "col"), P(), P("col", "row")),
        out_specs=(P("row", "col"), P("col", "row")),
        check_vma=False,
    )
```

```python
import functools

import jax
import jax.numpy as jnp
from jax import lax
from jax.experimental import pallas as pl
from jax.experimental.pallas import tpu as pltpu
from jax.sharding import PartitionSpec as P

MESH = pl.DeviceIdType.MESH
NN = ((1,), (0,))
NT = ((1,), (1,))
TN = ((0,), (0,))


def dot(left, right, dims=NN):
    return lax.dot_general(
        left, right, (dims, ((), ())), precision=lax.Precision.HIGH, preferred_element_type=jnp.float32
    )


def tdot(left, right):
    return dot(left, right, TN)


def halves(a):
    high = a.astype(jnp.bfloat16)
    return high, (a - high.astype(jnp.float32)).astype(jnp.bfloat16)


def dot3(left, right, dims):
    def one(a, b):
        return lax.dot_general(a, b, (dims, ((), ())), preferred_element_type=jnp.float32)

    (lh, ll), (rh, rl) = left, right
    return one(lh, rh) + (one(lh, rl) + one(ll, rh))


def whole_kernel(
    plan, x_hbm, y_hbm, t_hbm, s_hbm, vec_hbm, out_ref,
    xb, xt, y1b, y2b, sb, far_h, far_l, tb, vt, vst, w, gram, wf, tw, ybuf, zbuf, xs, xr, pt, pyb, pzb,
    ls, bulk_s, x_r, y_r, py_r, ry_r, rz_r, r_s, rx_s, rx_r, gz_r, gy_r, g_s, vp_r, vm_r, v_s,
):
    nz, q, nq, ahead, early, late, kept, sent, parts = plan
    half = nq * q
    must = [(i * q, q) for i in range(nq)]
    extras = early + late
    held = half + sum(n for _, n in extras)
    bw = x_hbm.shape[1]
    share = out_ref.shape[0]
    per = bw // share
    offs = [sum(parts[:g]) for g in range(len(parts))]
    spans = [(2 * per * o, 2 * per * n) for o, n in zip(offs, parts)]
    first_span = spans[0][1]
    wide = xt.shape[0]
    r, c = lax.axis_index("row"), lax.axis_index("col")
    z, y = r // 2, lax.rem(r, 2)
    x, k = c // 2, lax.rem(c, 2)
    mate = (r, c + 1 - 2 * k)
    peer = (r, c + 2 - 4 * x)
    peer_block = c + 2 - 4 * x
    ynext = (r + 1 - 2 * y, c)

    def zat(d):
        return lax.rem(z + d, nz)

    def znext(d):
        return (zat(d) * 2 + y, c)

    partners = [mate, peer, ynext] + [znext(d) for d in range(1, nz)]
    barrier = pltpu.get_barrier_semaphore()
    for other in partners:
        pl.semaphore_signal(barrier, inc=1, device_id=other, device_id_type=MESH)
    pl.semaphore_wait(barrier, len(partners))

    def send(src, dst, s, t, device):
        return pltpu.make_async_remote_copy(src, dst, s, t, device_id=device, device_id_type=MESH)

    def sent_all(ref, s):
        send(ref, ref, s, s, mate).wait_send()

    def arrive(ref, s):
        send(ref, ref, s, s, mate).wait_recv()

    def at(m):
        return pl.ds(m[0], m[1])

    def place(m, side):
        start, size = m
        base = side * half + start if start < half else (1 - side) * half + start - half
        return pl.ds(pl.multiple_of(base, 128), size)

    def lanes(b):
        return pl.ds(pl.multiple_of(b * bw, bw), bw)

    def index(m):
        return m[0] // q if m[0] < half else nq + extras.index(m)

    panels = (y1b, y2b)

    def x_local(m):
        return pltpu.make_async_copy(x_hbm.at[place(m, x)], xb.at[at(m), lanes(x)], x_r.at[index(m)])

    def x_peer(m):
        return send(x_hbm.at[place(m, 1 - x)], xb.at[at(m), lanes(x)], bulk_s.at[0], x_r.at[index(m)], peer)

    def y_local(p, m):
        return pltpu.make_async_copy(
            y_hbm.at[p, place(m, x)], panels[p].at[at(m), lanes(c)], y_r.at[p, index(m)])

    def y_peer(p, m):
        return send(
            y_hbm.at[p, place(m, 1 - x)], panels[p].at[at(m), lanes(c)], bulk_s.at[1], py_r.at[p, index(m)], peer)

    def y_mate(p, m):
        return send(
            y_hbm.at[p, place(m, x)], panels[p].at[at(m), lanes(c)], bulk_s.at[2], y_r.at[p, index(m)], mate)

    def y_forward(p, m):
        block = panels[p].at[at(m), lanes(peer_block)]
        return send(block, block, bulk_s.at[3], y_r.at[p, index(m)], mate)

    def wait_y(p, m):
        block = panels[p].at[at(m), pl.ds(0, 3 * bw)]
        pltpu.make_async_copy(block, block, y_r.at[p, index(m)]).wait()

    def pass_on(p, m):
        y_peer(p, m).wait_recv()
        y_forward(p, m).start()

    def send_bulk(m):
        x_peer(m).start()
        y_peer(1, m).start()
        y_peer(0, m).start()

    for m in must:
        x_peer(m).start()
        y_peer(1, m).start()
    for m in must[:ahead]:
        y_peer(0, m).start()
    for m in must + extras:
        x_local(m).start()
        for p in (1, 0):
            y_mate(p, m).start()
            y_local(p, m).start()
    t_copy = pltpu.make_async_copy(t_hbm, tb, ls.at[0])
    s_copy = pltpu.make_async_copy(s_hbm, sb, ls.at[1])
    t_copy.start()
    s_copy.start()

    w[...] = jnp.zeros_like(w)
    gram[...] = jnp.zeros_like(gram)
    pt[...] = jnp.zeros_like(pt)
    t_copy.wait()
    s_copy.wait()
    far = [(start + half, size) for start, size in sent]
    reach = far[0][0]
    for m in far:
        high, low = halves(sb[:, place(m, x)])
        far_h[:, m[0] - reach : m[0] - reach + m[1]] = high
        far_l[:, m[0] - reach : m[0] - reach + m[1]] = low

    def pieces(block, side):
        for o, n, (base, _) in zip(offs, parts, spans):
            for h in range(per):
                yield block + h * share + o, base + (side * per + h) * n, n

    def turn(m):
        pltpu.make_async_copy(xb.at[at(m)], xb.at[at(m)], x_r.at[index(m)]).wait()
        turned = xb[at(m), :].T
        for side in range(2):
            for src, dst, n in pieces(side * bw, side):
                xt[dst : dst + n, at(m)] = turned[src : src + n]

    def begin(m):
        turn(m)
        wait_y(1, m)
        w[0] += dot3(halves(xt[:, at(m)]), halves(y2b[at(m), :]), NN)

    for i, m in enumerate(must):
        pass_on(1, m)
        if i:
            begin(must[i - 1])
    begin(must[-1])

    class Sum:
        def __init__(self, n, piece, ys, zs, whole):
            self.n, self.piece, self.ys, self.zs, self.whole = n, piece, ys, zs, whole
            self.pending = list(range(1, nz))
            self.out = [
                send(piece(zat(d), 1 - y), ys(d), r_s.at[n], ry_r.at[n, d], ynext) for d in self.pending + [0]]
            self.hops = [send(piece(zat(d), y), zs(d), r_s.at[n], rz_r.at[n], znext(d)) for d in range(1, nz)]
            for copy in self.out:
                copy.start()

        def relay(self, count=nz):
            for d in self.pending[:count]:
                self.out[d - 1].wait_recv()
                self.piece(zat(d), y)[...] += self.ys(d)[...]
                self.hops[d - 1].start()
            self.pending = self.pending[count:]

        def total(self):
            self.out[-1].wait_recv()
            total = self.piece(z, y)[...] + self.ys(0)[...]
            arrive(self.whole(nz - 1), rz_r.at[self.n])
            for d in range(1, nz):
                total = total + self.zs(d)[...]
            return total

        def drain(self):
            sent_all(self.whole(2 * nz - 1), r_s.at[self.n])

    class AllSum:
        def __init__(self, n, panel, base, size):
            self.n = n
            rows = size // (2 * nz)
            self.rows = pl.ds(base // (2 * nz), rows)

            def block(ref, zz, yy):
                return ref.at[panel, pl.ds(pl.multiple_of(base + (zz * 2 + yy) * rows, 8), rows)]

            self.final = lambda zz, yy: block(wf, zz, yy)
            self.whole = lambda count: w.at[panel, pl.ds(0, count * rows)]
            self.panel = panel
            self.sum = Sum(
                n, lambda zz, yy: block(w, zz, yy),
                lambda d: ybuf.at[panel, d, self.rows], lambda d: zbuf.at[panel, d, self.rows], self.whole)
            self.relay = self.sum.relay

        def swap(self):
            n = self.n
            mine, other = xs.at[self.panel, self.rows], xr.at[self.panel, self.rows]
            mine[...] = self.sum.total()
            self.swapped = send(mine, other, rx_s.at[n], rx_r.at[n], peer)
            self.swapped.start()

        def gather(self):
            n = self.n
            self.swapped.wait_recv()
            mine = self.final(z, y)
            mine[...] = xs[self.panel, self.rows] + xr[self.panel, self.rows]
            self.along = [send(mine, mine, g_s.at[n], gz_r.at[n, d], znext(d)) for d in range(1, nz)]
            for copy in self.along:
                copy.start()
            self.across = [send(mine, mine, g_s.at[n], gy_r.at[n], ynext)]
            self.across[0].start()

        def forward(self):
            for d in range(1, nz):
                self.along[d - 1].wait_recv()
                block = self.final(lax.rem(z + nz - d, nz), y)
                self.across.append(send(block, block, g_s.at[self.n], gy_r.at[self.n], ynext))
                self.across[-1].start()

        def finish(self):
            arrive(self.whole(nz), gy_r.at[self.n])

        def drain(self):
            self.sum.drain()
            self.swapped.wait_send()
            sent_all(self.whole(2 * nz - 1), g_s.at[self.n])

    def inner(m):
        xt[:, at(m)] = xt[:, at(m)] - dot3(halves(tw[1]), halves(y2b[at(m), :]), NT)

    def raw(m):
        wait_y(0, m)
        first = halves(y1b[at(m), :])
        w[1] += dot3(halves(xt[:, at(m)]), first, NN)
        gram[...] += dot3(halves(y2b[at(m), :]), first, TN)

    a0 = AllSum(0, 0, 0, wide)
    a0.relay()
    a0.swap()
    for m in must[ahead:]:
        y_peer(0, m).start()
    for m in early:
        send_bulk(m)
    for m in must[:-2]:
        pass_on(0, m)
    for m in must[:-2]:
        raw(m)
    a0.gather()
    pass_on(0, must[-2])
    raw(must[-2])
    a0.forward()
    pass_on(0, must[-1])
    raw(must[-1])
    a0.finish()
    tw[1] = dot3(halves(wf[0]), halves(tb[1]), NT)
    w[1] = w[1] - dot3(halves(tw[1]), halves(gram[...]), NN)

    def take(m):
        pass_on(1, m)
        pass_on(0, m)

    def extra_inner(m):
        turn(m)
        wait_y(1, m)
        inner(m)

    a1 = AllSum(1, 1, 0, first_span)
    a2 = AllSum(2, 1, first_span, wide - first_span)
    a1.relay()
    for m in must[:2]:
        inner(m)
    a2.relay()
    a1.swap()
    for m in must[2:]:
        inner(m)
    a2.swap()
    for m in late:
        send_bulk(m)
    a1.gather()
    a2.gather()
    for m in early:
        take(m)
    a1.forward()
    a2.forward()

    def band(g):
        return pl.ds(*spans[g])

    later = pl.ds(first_span, wide - first_span)
    locals_ = sent + kept + extras

    def v_mate(b, rows, m):
        block = vt.at[k, rows, at(m)]
        slot = locals_.index(m) if m in locals_ else len(locals_) + b * len(far) + far.index(m)
        return send(block, block, v_s.at[1], vm_r.at[slot], mate)

    def v_peer(g, j):
        return send(vt.at[k, band(g), at(sent[j])], vt.at[k, band(g), at(far[j])], v_s.at[0], vp_r.at[g, j], peer)

    def v_out(m):
        return pltpu.make_async_copy(vst.at[at(m)], vec_hbm.at[place(m, x)], v_s.at[2])

    def write_out(m):
        for side in range(2):
            @pl.when(x == side)
            def _():
                block = [vt[k, dst : dst + n, at(m)] for _, dst, n in sorted(pieces(0, side))]
                vst[at(m), :] = jnp.concatenate(block, axis=0).T
        v_out(m).start()

    def weigh(rows):
        tw[0, rows, :] = dot3(halves(wf[1, rows, :]), halves(tb[0]), NT)

    def finish(rows, m):
        vt[k, rows, at(m)] = xt[rows, at(m)] - dot3(halves(tw[0, rows, :]), halves(y1b[at(m), :]), NT)

    a1.finish()
    weigh(band(0))
    for j, m in enumerate(sent):
        finish(band(0), m)
        v_peer(0, j).start()
    a2.finish()
    weigh(later)
    for j, m in enumerate(sent):
        finish(later, m)
        v_peer(1, j).start()
    for g in range(2, len(parts)):
        for j in range(len(sent)):
            v_peer(g, j).start()
    everything = pl.ds(0, wide)
    for m in sent:
        v_mate(0, everything, m).start()
    for m in kept:
        finish(everything, m)
        v_mate(0, everything, m).start()
    for m in late:
        take(m)
    for m in early:
        extra_inner(m)
        wait_y(0, m)
        finish(everything, m)
        v_mate(0, everything, m).start()

    def multiply(m):
        v_mate(0, everything, m).wait_recv()
        right = halves(sb[:, place(m, x)])
        for h in range(2):
            pt[h] += dot3(halves(vt[h, :, at(m)]), right, NT)

    for m in sent + kept:
        multiply(m)
    for m in late:
        extra_inner(m)
        wait_y(0, m)
        finish(everything, m)
        v_mate(0, everything, m).start()
    for m in extras:
        multiply(m)

    def multiply_far(g, j):
        m = far[j]
        cut = slice(m[0] - reach, m[0] - reach + m[1])
        both = vt[:, band(g), at(m)].reshape(2 * spans[g][1], m[1])
        added = dot3(halves(both), (far_h[:, cut], far_l[:, cut]), NT)
        pt[:, band(g), :] += added.reshape(2, spans[g][1], pt.shape[2])

    def scatter(g):
        n = parts[g]

        def piece(zz, yy):
            start = spans[g][0] + ((zz // 2) * per + yy) * n
            return pt.at[lax.rem(zz, 2), pl.ds(pl.multiple_of(start, 8), n)]

        def rows(ref):
            return lambda d: ref.at[d, pl.ds(offs[g], n)]

        return Sum(3 + g, piece, rows(pyb), rows(pzb), lambda count: sb.at[pl.ds(0, count * n), pl.ds(0, pt.shape[2])])

    def collect(g):
        out_ref[offs[g] : offs[g] + parts[g], :] = last[g].total()

    last = []
    todo = [(g, j) for g in range(len(parts)) for j in range(len(sent))]

    def arrived(g, j):
        v_mate(g, band(g), far[j]).wait_recv()
        multiply_far(g, j)
        if j == len(sent) - 1:
            last.append(scatter(g))
        elif g and j == len(sent) - 2:
            last[g - 1].relay()

    for t, (g, j) in enumerate(todo):
        v_peer(g, j).wait_recv()
        v_mate(g, band(g), far[j]).start()
        if t:
            arrived(*todo[t - 1])
        if t < len(locals_):
            write_out(locals_[t])
    arrived(*todo[-1])
    for m in locals_[len(todo):]:
        write_out(m)
    for one in last:
        one.relay()
    for m in far:
        write_out(m)
    for g in range(len(parts) - 1):
        collect(g)
    for s in (a0, a1, a2):
        s.drain()
    sent_all(x_hbm.at[pl.ds(0, held)], bulk_s.at[0])
    for i in (1, 2, 3):
        sent_all(y_hbm.at[:, pl.ds(0, held)], bulk_s.at[i])
    sent_all(vt.at[0, :, pl.ds(0, sum(n for _, n in sent))], v_s.at[0])
    sent_all(vt.at[0], v_s.at[1])
    pltpu.make_async_copy(vst, vec_hbm, v_s.at[2]).wait()
    collect(len(parts) - 1)
    for done in last:
        done.drain()


CHUNK = 4
AHEAD = 3
EARLY = (3,)
LATE = (2,)
PARTS = (2, 1, 1)
UNITS = 16
VMEM_BYTES = 54_000_000


def on_grid(nrow, ncol, eigvecs, reflectors, factors, slab):
    size, bw = eigvecs.shape
    panel = factors.shape[1]
    nz = nrow // 2
    half = size // 2
    unit = half // UNITS
    q = CHUNK * unit
    nq = half // q

    def ranges(start, sizes):
        out = []
        for n in sizes:
            out.append((start, n * unit))
            start += n * unit
        return out

    early = ranges(half, EARLY)
    late = ranges(half + sum(n for _, n in early), LATE)
    extra = sum(EARLY) + sum(LATE)
    kept = ranges(0, (extra,))
    first = (UNITS - extra) % CHUNK
    sent = ranges(extra * unit, ((first,) if first else ()) + (CHUNK,) * ((UNITS - extra) // CHUNK))
    held = half + extra * unit
    away = half - extra * unit
    wide = 2 * bw
    f32 = jnp.float32
    rows = wide // nrow
    mine = slab.shape[0]
    share = ncol * bw // nrow
    parts = tuple(n * share // sum(PARTS) for n in PARTS)
    g = len(parts)
    chunks = nq + len(EARLY) + len(LATE)
    slots = (1 + g) * len(sent) + len(kept) + len(EARLY) + len(LATE)
    sem = pltpu.SemaphoreType.DMA
    vmem = pltpu.VMEM
    vectors, product = pl.pallas_call(
        functools.partial(whole_kernel, (nz, q, nq, AHEAD, early, late, kept, sent, parts)),
        out_shape=(
            jax.ShapeDtypeStruct((size, bw), f32),
            jax.ShapeDtypeStruct((share, mine), f32),
        ),
        in_specs=[pl.BlockSpec(memory_space=pltpu.HBM)] * 4,
        out_specs=(pl.BlockSpec(memory_space=pl.ANY), pl.BlockSpec(memory_space=pltpu.VMEM)),
        scratch_shapes=[
            vmem((held, wide), f32), vmem((wide, held), f32), vmem((held, panel), f32), vmem((held, panel), f32),
            vmem(slab.shape, f32), vmem((mine, away), jnp.bfloat16), vmem((mine, away), jnp.bfloat16),
            vmem(factors.shape, f32), vmem((2, wide, size), f32), vmem((size, bw), f32),
            vmem((2, wide, panel), f32), vmem((panel, panel), f32),
            vmem((2, wide, panel), f32), vmem((2, wide, panel), f32),
            vmem((2, nz, rows, panel), f32), vmem((2, nz, rows, panel), f32),
            vmem((2, rows, panel), f32), vmem((2, rows, panel), f32),
            vmem((2, wide, mine), f32),
            vmem((nz, share, mine), f32), vmem((nz, share, mine), f32),
            sem((2,)), sem((4,)), sem((chunks,)), sem((2, chunks)), sem((2, chunks)),
            sem((3 + g, nz)), sem((3 + g,)), sem((3 + g,)), sem((3,)), sem((3,)),
            sem((3, nz)), sem((3,)), sem((3,)), sem((g, len(sent))), sem((slots,)), sem((3,)),
        ],
        compiler_params=pltpu.CompilerParams(
            collective_id=0, has_side_effects=True, vmem_limit_bytes=VMEM_BYTES),
        name="whole",
    )(eigvecs, reflectors, factors, slab)
    return vectors, product.T


def on_any(nrow, ncol, eigvecs, reflectors, factors, slab):
    c = lax.axis_index("col")
    first_own, second_own = reflectors[0], reflectors[1]
    all_x, second_y, first_y = (
        lax.all_gather(block, "col", axis=1, tiled=True) for block in (eigvecs, second_own, first_own)
    )
    own = second_own.shape[1]
    both = jnp.concatenate([second_own, first_own], axis=1)
    stacked = jnp.concatenate([tdot(both, all_x), tdot(first_own, second_y)])
    slab_x, slab_second, slab_first = (dot(block, slab, ((0,), (1,))) for block in (all_x, second_y, first_y))
    sums = lax.all_gather(lax.psum(stacked, "row"), "col")
    panel = factors.shape[1]
    second_w, first_raw, gram = (sums[:, i * own : (i + 1) * own].reshape(panel, -1) for i in range(3))
    second_tw = dot(factors[1], second_w)
    first_tw = dot(factors[0], first_raw - dot(gram, second_tw))
    partial = slab_x - tdot(second_tw, slab_second) - tdot(first_tw, slab_first)
    product = lax.psum_scatter(partial, "row", tiled=True)
    vectors = eigvecs
    for block, tw in ((second_y, second_tw), (first_y, first_tw)):
        width = eigvecs.shape[1]
        vectors = vectors - dot(block, lax.dynamic_slice_in_dim(tw, c * width, width, axis=1))
    return vectors, product.T


def solution(mesh):
    nrow, ncol = mesh.shape["row"], mesh.shape["col"]
    fits = ncol == 4 and nrow == 2 * ncol
    return jax.shard_map(
        functools.partial(on_grid if fits else on_any, nrow, ncol),
        mesh=mesh,
        in_specs=(P("row", "col"), P(None, "row", "col"), P(), P("col", "row")),
        out_specs=(P("row", "col"), P("col", "row")),
        check_vma=False,
    )
```

```python
import functools

import jax
import jax.numpy as jnp
from jax import lax
from jax.experimental import pallas as pl
from jax.experimental.pallas import tpu as pltpu
from jax.sharding import PartitionSpec as P

MESH = pl.DeviceIdType.MESH
NN = ((1,), (0,))
NT = ((1,), (1,))
TN = ((0,), (0,))


def dot(left, right, dims=NN):
    return lax.dot_general(
        left, right, (dims, ((), ())), precision=lax.Precision.HIGH, preferred_element_type=jnp.float32
    )


def tdot(left, right):
    return dot(left, right, TN)


def halves(a):
    high = a.astype(jnp.bfloat16)
    return high, (a - high.astype(jnp.float32)).astype(jnp.bfloat16)


def dot3(left, right, dims):
    def one(a, b):
        return lax.dot_general(a, b, (dims, ((), ())), preferred_element_type=jnp.float32)

    (lh, ll), (rh, rl) = left, right
    return one(lh, rh) + (one(lh, rl) + one(ll, rh))


def whole_kernel(
    plan, x_hbm, y_hbm, t_hbm, s_hbm, vec_hbm, out_ref,
    xb, xt, y1b, y2b, sb, far_h, far_l, tb, vt, vst, w, gram, wf, tw, ybuf, zbuf, xs, xr, pt, pyb, pzb,
    ls, bulk_s, x_r, y_r, py_r, ry_r, rz_r, r_s, rx_s, rx_r, gz_r, gy_r, g_s, vp_r, vm_r, v_s,
):
    nz, q, nq, ahead, early, late, kept, sent, parts = plan
    half = nq * q
    must = [(i * q, q) for i in range(nq)]
    extras = early + late
    held = half + sum(n for _, n in extras)
    bw = x_hbm.shape[1]
    share = out_ref.shape[0]
    per = bw // share
    offs = [sum(parts[:g]) for g in range(len(parts))]
    spans = [(2 * per * o, 2 * per * n) for o, n in zip(offs, parts)]
    first_span = spans[0][1]
    wide = xt.shape[0]
    r, c = lax.axis_index("row"), lax.axis_index("col")
    z, y = r // 2, lax.rem(r, 2)
    x, k = c // 2, lax.rem(c, 2)
    mate = (r, c + 1 - 2 * k)
    peer = (r, c + 2 - 4 * x)
    peer_block = c + 2 - 4 * x
    ynext = (r + 1 - 2 * y, c)

    def zat(d):
        return lax.rem(z + d, nz)

    def znext(d):
        return (zat(d) * 2 + y, c)

    partners = [mate, peer, ynext] + [znext(d) for d in range(1, nz)]
    barrier = pltpu.get_barrier_semaphore()
    for other in partners:
        pl.semaphore_signal(barrier, inc=1, device_id=other, device_id_type=MESH)
    pl.semaphore_wait(barrier, len(partners))

    def send(src, dst, s, t, device):
        return pltpu.make_async_remote_copy(src, dst, s, t, device_id=device, device_id_type=MESH)

    def sent_all(ref, s):
        send(ref, ref, s, s, mate).wait_send()

    def arrive(ref, s):
        send(ref, ref, s, s, mate).wait_recv()

    def at(m):
        return pl.ds(m[0], m[1])

    def place(m, side):
        start, size = m
        base = side * half + start if start < half else (1 - side) * half + start - half
        return pl.ds(pl.multiple_of(base, 128), size)

    def lanes(b):
        return pl.ds(pl.multiple_of(b * bw, bw), bw)

    def index(m):
        return m[0] // q if m[0] < half else nq + extras.index(m)

    panels = (y1b, y2b)

    def x_local(m):
        return pltpu.make_async_copy(x_hbm.at[place(m, x)], xb.at[at(m), lanes(x)], x_r.at[index(m)])

    def x_peer(m, slot):
        return send(x_hbm.at[place(m, 1 - x)], xb.at[at(m), lanes(x)], bulk_s.at[0], x_r.at[slot], peer)

    def y_local(p, m):
        return pltpu.make_async_copy(
            y_hbm.at[p, place(m, x)], panels[p].at[at(m), lanes(c)], y_r.at[p, index(m)])

    def y_peer(p, m, slot):
        return send(
            y_hbm.at[p, place(m, 1 - x)], panels[p].at[at(m), lanes(c)], bulk_s.at[1], py_r.at[p, slot], peer)

    def y_mate(p, m):
        return send(
            y_hbm.at[p, place(m, x)], panels[p].at[at(m), lanes(c)], bulk_s.at[2], y_r.at[p, index(m)], mate)

    def y_forward(p, m):
        block = panels[p].at[at(m), lanes(peer_block)]
        return send(block, block, bulk_s.at[3], y_r.at[p, index(m)], mate)

    def wait_y(p, m):
        block = panels[p].at[at(m), pl.ds(0, 3 * bw)]
        pltpu.make_async_copy(block, block, y_r.at[p, index(m)]).wait()

    def pass_on(p, m):
        y_peer(p, m, index(m)).wait_recv()
        y_forward(p, m).start()

    def cut(m):
        n = m[1] // CUTS
        return [(m[0] + i * n, n) for i in range(CUTS)]

    def send_x(m):
        for part in cut(m):
            x_peer(part, index(m)).start()

    def send_y(p, m):
        for part in cut(m):
            y_peer(p, part, index(m)).start()

    def send_bulk(m):
        send_x(m)
        send_y(1, m)
        send_y(0, m)

    for m in must:
        send_x(m)
        send_y(1, m)
    for m in must[:ahead]:
        send_y(0, m)
    for m in must + extras:
        x_local(m).start()
        for p in (1, 0):
            y_mate(p, m).start()
            y_local(p, m).start()
    t_copy = pltpu.make_async_copy(t_hbm, tb, ls.at[0])
    s_copy = pltpu.make_async_copy(s_hbm, sb, ls.at[1])
    t_copy.start()
    s_copy.start()

    w[...] = jnp.zeros_like(w)
    gram[...] = jnp.zeros_like(gram)
    pt[...] = jnp.zeros_like(pt)
    t_copy.wait()
    s_copy.wait()
    far = [(start + half, size) for start, size in sent]
    reach = far[0][0]
    for m in far:
        high, low = halves(sb[:, place(m, x)])
        far_h[:, m[0] - reach : m[0] - reach + m[1]] = high
        far_l[:, m[0] - reach : m[0] - reach + m[1]] = low

    def pieces(block, side):
        for o, n, (base, _) in zip(offs, parts, spans):
            for h in range(per):
                yield block + h * share + o, base + (side * per + h) * n, n

    def turn(m):
        pltpu.make_async_copy(xb.at[at(m)], xb.at[at(m)], x_r.at[index(m)]).wait()
        turned = xb[at(m), :].T
        for side in range(2):
            for src, dst, n in pieces(side * bw, side):
                xt[dst : dst + n, at(m)] = turned[src : src + n]

    def begin(m):
        turn(m)
        wait_y(1, m)
        w[0] += dot3(halves(xt[:, at(m)]), halves(y2b[at(m), :]), NN)

    for i, m in enumerate(must):
        pass_on(1, m)
        if i:
            begin(must[i - 1])
    begin(must[-1])

    class Sum:
        def __init__(self, n, piece, ys, zs, whole):
            self.n, self.piece, self.ys, self.zs, self.whole = n, piece, ys, zs, whole
            self.pending = list(range(1, nz))
            self.out = [
                send(piece(zat(d), 1 - y), ys(d), r_s.at[n], ry_r.at[n, d], ynext) for d in self.pending + [0]]
            self.hops = [send(piece(zat(d), y), zs(d), r_s.at[n], rz_r.at[n], znext(d)) for d in range(1, nz)]
            for copy in self.out:
                copy.start()

        def relay(self, count=nz):
            for d in self.pending[:count]:
                self.out[d - 1].wait_recv()
                self.piece(zat(d), y)[...] += self.ys(d)[...]
                self.hops[d - 1].start()
            self.pending = self.pending[count:]

        def total(self):
            self.out[-1].wait_recv()
            total = self.piece(z, y)[...] + self.ys(0)[...]
            arrive(self.whole(nz - 1), rz_r.at[self.n])
            for d in range(1, nz):
                total = total + self.zs(d)[...]
            return total

        def drain(self):
            sent_all(self.whole(2 * nz - 1), r_s.at[self.n])

    class AllSum:
        def __init__(self, n, panel, base, size):
            self.n = n
            rows = size // (2 * nz)
            self.rows = pl.ds(base // (2 * nz), rows)

            def block(ref, zz, yy):
                return ref.at[panel, pl.ds(pl.multiple_of(base + (zz * 2 + yy) * rows, 8), rows)]

            self.final = lambda zz, yy: block(wf, zz, yy)
            self.whole = lambda count: w.at[panel, pl.ds(0, count * rows)]
            self.panel = panel
            self.sum = Sum(
                n, lambda zz, yy: block(w, zz, yy),
                lambda d: ybuf.at[panel, d, self.rows], lambda d: zbuf.at[panel, d, self.rows], self.whole)
            self.relay = self.sum.relay

        def swap(self):
            n = self.n
            mine, other = xs.at[self.panel, self.rows], xr.at[self.panel, self.rows]
            mine[...] = self.sum.total()
            self.swapped = send(mine, other, rx_s.at[n], rx_r.at[n], peer)
            self.swapped.start()

        def gather(self):
            n = self.n
            self.swapped.wait_recv()
            mine = self.final(z, y)
            mine[...] = xs[self.panel, self.rows] + xr[self.panel, self.rows]
            self.along = [send(mine, mine, g_s.at[n], gz_r.at[n, d], znext(d)) for d in range(1, nz)]
            for copy in self.along:
                copy.start()
            self.across = [send(mine, mine, g_s.at[n], gy_r.at[n], ynext)]
            self.across[0].start()

        def forward(self):
            for d in range(1, nz):
                self.along[d - 1].wait_recv()
                block = self.final(lax.rem(z + nz - d, nz), y)
                self.across.append(send(block, block, g_s.at[self.n], gy_r.at[self.n], ynext))
                self.across[-1].start()

        def finish(self):
            arrive(self.whole(nz), gy_r.at[self.n])

        def drain(self):
            self.sum.drain()
            self.swapped.wait_send()
            sent_all(self.whole(2 * nz - 1), g_s.at[self.n])

    def inner(m):
        xt[:, at(m)] = xt[:, at(m)] - dot3(halves(tw[1]), halves(y2b[at(m), :]), NT)

    def raw(m):
        wait_y(0, m)
        first = halves(y1b[at(m), :])
        w[1] += dot3(halves(xt[:, at(m)]), first, NN)
        gram[...] += dot3(halves(y2b[at(m), :]), first, TN)

    a0 = AllSum(0, 0, 0, wide)
    a0.relay()
    a0.swap()
    for m in must[ahead:]:
        send_y(0, m)
    for m in early:
        send_bulk(m)
    for m in must[:-2]:
        pass_on(0, m)
    for m in must[:-2]:
        raw(m)
    a0.gather()
    pass_on(0, must[-2])
    raw(must[-2])
    a0.forward()
    pass_on(0, must[-1])
    raw(must[-1])
    a0.finish()
    tw[1] = dot3(halves(wf[0]), halves(tb[1]), NT)
    w[1] = w[1] - dot3(halves(tw[1]), halves(gram[...]), NN)

    def take(m):
        pass_on(1, m)
        pass_on(0, m)

    def extra_inner(m):
        turn(m)
        wait_y(1, m)
        inner(m)

    a1 = AllSum(1, 1, 0, first_span)
    a2 = AllSum(2, 1, first_span, wide - first_span)
    a1.relay()
    for m in must[:2]:
        inner(m)
    a2.relay()
    a1.swap()
    for m in must[2:]:
        inner(m)
    a2.swap()
    for m in late:
        send_bulk(m)
    a1.gather()
    a2.gather()
    for m in early:
        take(m)
    a1.forward()
    a2.forward()

    def band(g):
        return pl.ds(*spans[g])

    later = pl.ds(first_span, wide - first_span)
    locals_ = sent + kept + extras

    def v_mate(b, rows, m):
        block = vt.at[k, rows, at(m)]
        slot = locals_.index(m) if m in locals_ else len(locals_) + b * len(far) + far.index(m)
        return send(block, block, v_s.at[1], vm_r.at[slot], mate)

    def v_peer(g, j):
        return send(vt.at[k, band(g), at(sent[j])], vt.at[k, band(g), at(far[j])], v_s.at[0], vp_r.at[g, j], peer)

    def v_out(m):
        return pltpu.make_async_copy(vst.at[at(m)], vec_hbm.at[place(m, x)], v_s.at[2])

    def write_out(m):
        for side in range(2):
            @pl.when(x == side)
            def _():
                block = [vt[k, dst : dst + n, at(m)] for _, dst, n in sorted(pieces(0, side))]
                vst[at(m), :] = jnp.concatenate(block, axis=0).T
        v_out(m).start()

    def weigh(rows):
        tw[0, rows, :] = dot3(halves(wf[1, rows, :]), halves(tb[0]), NT)

    def finish(rows, m):
        vt[k, rows, at(m)] = xt[rows, at(m)] - dot3(halves(tw[0, rows, :]), halves(y1b[at(m), :]), NT)

    a1.finish()
    weigh(band(0))
    for j, m in enumerate(sent):
        finish(band(0), m)
        v_peer(0, j).start()
    a2.finish()
    weigh(later)
    for j, m in enumerate(sent):
        finish(later, m)
        v_peer(1, j).start()
    for g in range(2, len(parts)):
        for j in range(len(sent)):
            v_peer(g, j).start()
    everything = pl.ds(0, wide)
    for m in sent:
        v_mate(0, everything, m).start()
    for m in kept:
        finish(everything, m)
        v_mate(0, everything, m).start()
    for m in late:
        take(m)
    for m in early:
        extra_inner(m)
        wait_y(0, m)
        finish(everything, m)
        v_mate(0, everything, m).start()

    def multiply(m):
        v_mate(0, everything, m).wait_recv()
        right = halves(sb[:, place(m, x)])
        for h in range(2):
            pt[h] += dot3(halves(vt[h, :, at(m)]), right, NT)

    for m in sent + kept:
        multiply(m)
    for m in late:
        extra_inner(m)
        wait_y(0, m)
        finish(everything, m)
        v_mate(0, everything, m).start()
    for m in extras:
        multiply(m)

    def multiply_far(g, j):
        m = far[j]
        cut = slice(m[0] - reach, m[0] - reach + m[1])
        both = vt[:, band(g), at(m)].reshape(2 * spans[g][1], m[1])
        added = dot3(halves(both), (far_h[:, cut], far_l[:, cut]), NT)
        pt[:, band(g), :] += added.reshape(2, spans[g][1], pt.shape[2])

    def scatter(g):
        n = parts[g]

        def piece(zz, yy):
            start = spans[g][0] + ((zz // 2) * per + yy) * n
            return pt.at[lax.rem(zz, 2), pl.ds(pl.multiple_of(start, 8), n)]

        def rows(ref):
            return lambda d: ref.at[d, pl.ds(offs[g], n)]

        return Sum(3 + g, piece, rows(pyb), rows(pzb), lambda count: sb.at[pl.ds(0, count * n), pl.ds(0, pt.shape[2])])

    def collect(g):
        out_ref[offs[g] : offs[g] + parts[g], :] = last[g].total()

    last = []
    todo = [(g, j) for g in range(len(parts)) for j in range(len(sent))]

    def arrived(g, j):
        v_mate(g, band(g), far[j]).wait_recv()
        multiply_far(g, j)
        if j == len(sent) - 1:
            last.append(scatter(g))
        elif g and j == len(sent) - 2 and g < len(parts) - 1:
            last[g - 1].relay()

    for t, (g, j) in enumerate(todo):
        v_peer(g, j).wait_recv()
        v_mate(g, band(g), far[j]).start()
        if t:
            arrived(*todo[t - 1])
        if t < len(locals_):
            write_out(locals_[t])
    arrived(*todo[-1])
    for m in locals_[len(todo):]:
        write_out(m)
    for one in last:
        one.relay()
    for m in far:
        write_out(m)
    for g in range(len(parts) - 1):
        collect(g)
    for s in (a0, a1, a2):
        s.drain()
    sent_all(x_hbm.at[pl.ds(0, held)], bulk_s.at[0])
    for i in (1, 2, 3):
        sent_all(y_hbm.at[:, pl.ds(0, held)], bulk_s.at[i])
    sent_all(vt.at[0, :, pl.ds(0, sum(n for _, n in sent))], v_s.at[0])
    sent_all(vt.at[0], v_s.at[1])
    pltpu.make_async_copy(vst, vec_hbm, v_s.at[2]).wait()
    collect(len(parts) - 1)
    for done in last:
        done.drain()


CUTS = 2
CHUNK = 4
AHEAD = 3
EARLY = (4,)
LATE = (2,)
PARTS = (2, 1, 1)
UNITS = 16
VMEM_BYTES = 54_000_000


def on_grid(nrow, ncol, eigvecs, reflectors, factors, slab):
    size, bw = eigvecs.shape
    panel = factors.shape[1]
    nz = nrow // 2
    half = size // 2
    unit = half // UNITS
    q = CHUNK * unit
    nq = half // q

    def ranges(start, sizes):
        out = []
        for n in sizes:
            out.append((start, n * unit))
            start += n * unit
        return out

    early = ranges(half, EARLY)
    late = ranges(half + sum(n for _, n in early), LATE)
    extra = sum(EARLY) + sum(LATE)
    kept = ranges(0, (extra,))
    rest = (UNITS - extra) % CHUNK
    sent = ranges(extra * unit, (CHUNK,) * ((UNITS - extra) // CHUNK) + ((rest,) if rest else ()))
    held = half + extra * unit
    away = half - extra * unit
    wide = 2 * bw
    f32 = jnp.float32
    rows = wide // nrow
    mine = slab.shape[0]
    share = ncol * bw // nrow
    parts = tuple(n * share // sum(PARTS) for n in PARTS)
    g = len(parts)
    chunks = nq + len(EARLY) + len(LATE)
    slots = (1 + g) * len(sent) + len(kept) + len(EARLY) + len(LATE)
    sem = pltpu.SemaphoreType.DMA
    vmem = pltpu.VMEM
    vectors, product = pl.pallas_call(
        functools.partial(whole_kernel, (nz, q, nq, AHEAD, early, late, kept, sent, parts)),
        out_shape=(
            jax.ShapeDtypeStruct((size, bw), f32),
            jax.ShapeDtypeStruct((share, mine), f32),
        ),
        in_specs=[pl.BlockSpec(memory_space=pltpu.HBM)] * 4,
        out_specs=(pl.BlockSpec(memory_space=pl.ANY), pl.BlockSpec(memory_space=pltpu.VMEM)),
        scratch_shapes=[
            vmem((held, wide), f32), vmem((wide, held), f32), vmem((held, panel), f32), vmem((held, panel), f32),
            vmem(slab.shape, f32), vmem((mine, away), jnp.bfloat16), vmem((mine, away), jnp.bfloat16),
            vmem(factors.shape, f32), vmem((2, wide, size), f32), vmem((size, bw), f32),
            vmem((2, wide, panel), f32), vmem((panel, panel), f32),
            vmem((2, wide, panel), f32), vmem((2, wide, panel), f32),
            vmem((2, nz, rows, panel), f32), vmem((2, nz, rows, panel), f32),
            vmem((2, rows, panel), f32), vmem((2, rows, panel), f32),
            vmem((2, wide, mine), f32),
            vmem((nz, share, mine), f32), vmem((nz, share, mine), f32),
            sem((2,)), sem((4,)), sem((chunks,)), sem((2, chunks)), sem((2, chunks)),
            sem((3 + g, nz)), sem((3 + g,)), sem((3 + g,)), sem((3,)), sem((3,)),
            sem((3, nz)), sem((3,)), sem((3,)), sem((g, len(sent))), sem((slots,)), sem((3,)),
        ],
        compiler_params=pltpu.CompilerParams(
            collective_id=0, has_side_effects=True, vmem_limit_bytes=VMEM_BYTES),
        name="whole",
    )(eigvecs, reflectors, factors, slab)
    return vectors, product.T


def on_any(nrow, ncol, eigvecs, reflectors, factors, slab):
    c = lax.axis_index("col")
    first_own, second_own = reflectors[0], reflectors[1]
    all_x, second_y, first_y = (
        lax.all_gather(block, "col", axis=1, tiled=True) for block in (eigvecs, second_own, first_own)
    )
    own = second_own.shape[1]
    both = jnp.concatenate([second_own, first_own], axis=1)
    stacked = jnp.concatenate([tdot(both, all_x), tdot(first_own, second_y)])
    slab_x, slab_second, slab_first = (dot(block, slab, ((0,), (1,))) for block in (all_x, second_y, first_y))
    sums = lax.all_gather(lax.psum(stacked, "row"), "col")
    panel = factors.shape[1]
    second_w, first_raw, gram = (sums[:, i * own : (i + 1) * own].reshape(panel, -1) for i in range(3))
    second_tw = dot(factors[1], second_w)
    first_tw = dot(factors[0], first_raw - dot(gram, second_tw))
    partial = slab_x - tdot(second_tw, slab_second) - tdot(first_tw, slab_first)
    product = lax.psum_scatter(partial, "row", tiled=True)
    vectors = eigvecs
    for block, tw in ((second_y, second_tw), (first_y, first_tw)):
        width = eigvecs.shape[1]
        vectors = vectors - dot(block, lax.dynamic_slice_in_dim(tw, c * width, width, axis=1))
    return vectors, product.T


def solution(mesh):
    nrow, ncol = mesh.shape["row"], mesh.shape["col"]
    fits = ncol == 4 and nrow == 2 * ncol
    return jax.shard_map(
        functools.partial(on_grid if fits else on_any, nrow, ncol),
        mesh=mesh,
        in_specs=(P("row", "col"), P(None, "row", "col"), P(), P("col", "row")),
        out_specs=(P("row", "col"), P("col", "row")),
        check_vma=False,
    )
```

```python
import functools

import jax
import jax.numpy as jnp
from jax import lax
from jax.experimental import pallas as pl
from jax.experimental.pallas import tpu as pltpu
from jax.sharding import PartitionSpec as P

MESH = pl.DeviceIdType.MESH
NN = ((1,), (0,))
NT = ((1,), (1,))
TN = ((0,), (0,))


def dot(left, right, dims=NN):
    return lax.dot_general(
        left, right, (dims, ((), ())), precision=lax.Precision.HIGH, preferred_element_type=jnp.float32
    )


def tdot(left, right):
    return dot(left, right, TN)


def halves(a):
    high = a.astype(jnp.bfloat16)
    return high, (a - high.astype(jnp.float32)).astype(jnp.bfloat16)


def dot3(left, right, dims):
    def one(a, b):
        return lax.dot_general(a, b, (dims, ((), ())), preferred_element_type=jnp.float32)

    (lh, ll), (rh, rl) = left, right
    free = 1 - dims[0][0]
    size = lh.shape[free]
    if size > STACK:
        return one(lh, rh) + (one(lh, rl) + one(ll, rh))
    stacked = one(jnp.concatenate([lh, ll], axis=free), rh)
    return stacked[:size] + (one(lh, rl) + stacked[size:])


STACK = 256


def whole_kernel(
    plan, x_hbm, y_hbm, t_hbm, s_hbm, vec_hbm, out_ref,
    xb, xt, y1b, y2b, sb, far_h, far_l, tb, vt, vst, w, gram, wf, tw, ybuf, zbuf, xs, xr, pt, pyb, pzb,
    ls, bulk_s, x_r, y_r, py_r, ry_r, rz_r, r_s, rx_s, rx_r, gz_r, gy_r, g_s, vp_r, vm_r, v_s,
):
    nz, q, nq, ahead, early, late, kept, sent, parts = plan
    half = nq * q
    must = [(i * q, q) for i in range(nq)]
    extras = early + late
    held = half + sum(n for _, n in extras)
    bw = x_hbm.shape[1]
    share = out_ref.shape[0]
    per = bw // share
    offs = [sum(parts[:g]) for g in range(len(parts))]
    spans = [(2 * per * o, 2 * per * n) for o, n in zip(offs, parts)]
    first_span = spans[0][1]
    wide = xt.shape[0]
    r, c = lax.axis_index("row"), lax.axis_index("col")
    z, y = r // 2, lax.rem(r, 2)
    x, k = c // 2, lax.rem(c, 2)
    mate = (r, c + 1 - 2 * k)
    peer = (r, c + 2 - 4 * x)
    peer_block = c + 2 - 4 * x
    ynext = (r + 1 - 2 * y, c)

    def zat(d):
        return lax.rem(z + d, nz)

    def znext(d):
        return (zat(d) * 2 + y, c)

    partners = [mate, peer, ynext] + [znext(d) for d in range(1, nz)]
    barrier = pltpu.get_barrier_semaphore()
    for other in partners:
        pl.semaphore_signal(barrier, inc=1, device_id=other, device_id_type=MESH)
    pl.semaphore_wait(barrier, len(partners))

    def send(src, dst, s, t, device):
        return pltpu.make_async_remote_copy(src, dst, s, t, device_id=device, device_id_type=MESH)

    def sent_all(ref, s):
        send(ref, ref, s, s, mate).wait_send()

    def arrive(ref, s):
        send(ref, ref, s, s, mate).wait_recv()

    def at(m):
        return pl.ds(m[0], m[1])

    def place(m, side):
        start, size = m
        base = side * half + start if start < half else (1 - side) * half + start - half
        return pl.ds(pl.multiple_of(base, 128), size)

    def lanes(b):
        return pl.ds(pl.multiple_of(b * bw, bw), bw)

    def index(m):
        return m[0] // q if m[0] < half else nq + extras.index(m)

    panels = (y1b, y2b)

    def x_local(m):
        return pltpu.make_async_copy(x_hbm.at[place(m, x)], xb.at[at(m), lanes(x)], x_r.at[index(m)])

    def x_peer(m, slot):
        return send(x_hbm.at[place(m, 1 - x)], xb.at[at(m), lanes(x)], bulk_s.at[0], x_r.at[slot], peer)

    def y_local(p, m):
        return pltpu.make_async_copy(
            y_hbm.at[p, place(m, x)], panels[p].at[at(m), lanes(c)], y_r.at[p, index(m)])

    def y_peer(p, m, slot):
        return send(
            y_hbm.at[p, place(m, 1 - x)], panels[p].at[at(m), lanes(c)], bulk_s.at[1], py_r.at[p, slot], peer)

    def y_mate(p, m):
        return send(
            y_hbm.at[p, place(m, x)], panels[p].at[at(m), lanes(c)], bulk_s.at[2], y_r.at[p, index(m)], mate)

    def y_forward(p, m):
        block = panels[p].at[at(m), lanes(peer_block)]
        return send(block, block, bulk_s.at[3], y_r.at[p, index(m)], mate)

    def wait_y(p, m):
        block = panels[p].at[at(m), pl.ds(0, 3 * bw)]
        pltpu.make_async_copy(block, block, y_r.at[p, index(m)]).wait()

    def pass_on(p, m):
        y_peer(p, m, index(m)).wait_recv()
        y_forward(p, m).start()

    def cut(m):
        n = m[1] // CUTS
        return [(m[0] + i * n, n) for i in range(CUTS)]

    def send_x(m):
        for part in cut(m):
            x_peer(part, index(m)).start()

    def send_y(p, m):
        for part in cut(m):
            y_peer(p, part, index(m)).start()

    def send_bulk(m):
        send_x(m)
        send_y(1, m)
        send_y(0, m)

    for m in must:
        send_x(m)
        send_y(1, m)
    for m in must[:ahead]:
        send_y(0, m)
    for m in must + extras:
        x_local(m).start()
        for p in (1, 0):
            y_mate(p, m).start()
            y_local(p, m).start()
    t_copy = pltpu.make_async_copy(t_hbm, tb, ls.at[0])
    s_copy = pltpu.make_async_copy(s_hbm, sb, ls.at[1])
    t_copy.start()
    s_copy.start()

    w[...] = jnp.zeros_like(w)
    gram[...] = jnp.zeros_like(gram)
    pt[...] = jnp.zeros_like(pt)
    t_copy.wait()
    s_copy.wait()
    far = [(start + half, size) for start, size in sent]
    reach = far[0][0]
    for m in far:
        high, low = halves(sb[:, place(m, x)])
        far_h[:, m[0] - reach : m[0] - reach + m[1]] = high
        far_l[:, m[0] - reach : m[0] - reach + m[1]] = low

    def pieces(block, side):
        for o, n, (base, _) in zip(offs, parts, spans):
            for h in range(per):
                yield block + h * share + o, base + (side * per + h) * n, n

    def turn(m):
        pltpu.make_async_copy(xb.at[at(m)], xb.at[at(m)], x_r.at[index(m)]).wait()
        turned = xb[at(m), :].T
        for side in range(2):
            for src, dst, n in pieces(side * bw, side):
                xt[dst : dst + n, at(m)] = turned[src : src + n]

    def begin(m):
        turn(m)
        wait_y(1, m)
        w[0] += dot3(halves(xt[:, at(m)]), halves(y2b[at(m), :]), NN)

    for i, m in enumerate(must):
        pass_on(1, m)
        if i:
            begin(must[i - 1])
    begin(must[-1])

    class Sum:
        def __init__(self, n, piece, ys, zs, whole):
            self.n, self.piece, self.ys, self.zs, self.whole = n, piece, ys, zs, whole
            self.pending = list(range(1, nz))
            self.out = [
                send(piece(zat(d), 1 - y), ys(d), r_s.at[n], ry_r.at[n, d], ynext) for d in self.pending + [0]]
            self.hops = [send(piece(zat(d), y), zs(d), r_s.at[n], rz_r.at[n], znext(d)) for d in range(1, nz)]
            for copy in self.out:
                copy.start()

        def relay(self, count=nz):
            for d in self.pending[:count]:
                self.out[d - 1].wait_recv()
                self.piece(zat(d), y)[...] += self.ys(d)[...]
                self.hops[d - 1].start()
            self.pending = self.pending[count:]

        def total(self):
            self.out[-1].wait_recv()
            total = self.piece(z, y)[...] + self.ys(0)[...]
            arrive(self.whole(nz - 1), rz_r.at[self.n])
            for d in range(1, nz):
                total = total + self.zs(d)[...]
            return total

        def drain(self):
            sent_all(self.whole(2 * nz - 1), r_s.at[self.n])

    class AllSum:
        def __init__(self, n, panel, base, size):
            self.n = n
            rows = size // (2 * nz)
            self.rows = pl.ds(base // (2 * nz), rows)

            def block(ref, zz, yy):
                return ref.at[panel, pl.ds(pl.multiple_of(base + (zz * 2 + yy) * rows, 8), rows)]

            self.final = lambda zz, yy: block(wf, zz, yy)
            self.whole = lambda count: w.at[panel, pl.ds(0, count * rows)]
            self.panel = panel
            self.sum = Sum(
                n, lambda zz, yy: block(w, zz, yy),
                lambda d: ybuf.at[panel, d, self.rows], lambda d: zbuf.at[panel, d, self.rows], self.whole)
            self.relay = self.sum.relay

        def swap(self):
            n = self.n
            mine, other = xs.at[self.panel, self.rows], xr.at[self.panel, self.rows]
            mine[...] = self.sum.total()
            self.swapped = send(mine, other, rx_s.at[n], rx_r.at[n], peer)
            self.swapped.start()

        def gather(self):
            n = self.n
            self.swapped.wait_recv()
            mine = self.final(z, y)
            mine[...] = xs[self.panel, self.rows] + xr[self.panel, self.rows]
            self.along = [send(mine, mine, g_s.at[n], gz_r.at[n, d], znext(d)) for d in range(1, nz)]
            for copy in self.along:
                copy.start()
            self.across = [send(mine, mine, g_s.at[n], gy_r.at[n], ynext)]
            self.across[0].start()

        def forward(self):
            for d in range(1, nz):
                self.along[d - 1].wait_recv()
                block = self.final(lax.rem(z + nz - d, nz), y)
                self.across.append(send(block, block, g_s.at[self.n], gy_r.at[self.n], ynext))
                self.across[-1].start()

        def finish(self):
            arrive(self.whole(nz), gy_r.at[self.n])

        def drain(self):
            self.sum.drain()
            self.swapped.wait_send()
            sent_all(self.whole(2 * nz - 1), g_s.at[self.n])

    def inner(m):
        xt[:, at(m)] = xt[:, at(m)] - dot3(halves(tw[1]), halves(y2b[at(m), :]), NT)

    def raw(m):
        wait_y(0, m)
        first = halves(y1b[at(m), :])
        w[1] += dot3(halves(xt[:, at(m)]), first, NN)
        gram[...] += dot3(halves(y2b[at(m), :]), first, TN)

    a0 = AllSum(0, 0, 0, wide)
    a0.relay()
    a0.swap()
    for m in must[ahead:]:
        send_y(0, m)
    for m in early:
        send_bulk(m)
    for m in must[:-2]:
        pass_on(0, m)
    for m in must[:-2]:
        raw(m)
    a0.gather()
    pass_on(0, must[-2])
    raw(must[-2])
    a0.forward()
    pass_on(0, must[-1])
    raw(must[-1])
    a0.finish()
    tw[1] = dot3(halves(wf[0]), halves(tb[1]), NT)
    w[1] = w[1] - dot3(halves(tw[1]), halves(gram[...]), NN)

    def take(m):
        pass_on(1, m)
        pass_on(0, m)

    def extra_inner(m):
        turn(m)
        wait_y(1, m)
        inner(m)

    a1 = AllSum(1, 1, 0, first_span)
    a2 = AllSum(2, 1, first_span, wide - first_span)
    a1.relay()
    for m in must[:2]:
        inner(m)
    a2.relay()
    a1.swap()
    for m in must[2:]:
        inner(m)
    a2.swap()
    for m in late:
        send_bulk(m)
    a1.gather()
    a2.gather()
    for m in early:
        take(m)
    a1.forward()
    a2.forward()
    for m in early:
        extra_inner(m)

    def band(g):
        return pl.ds(*spans[g])

    later = pl.ds(first_span, wide - first_span)
    locals_ = sent + kept + extras

    def v_mate(b, rows, m):
        block = vt.at[k, rows, at(m)]
        slot = locals_.index(m) if m in locals_ else len(locals_) + b * len(far) + far.index(m)
        return send(block, block, v_s.at[1], vm_r.at[slot], mate)

    def v_peer(g, j):
        return send(vt.at[k, band(g), at(sent[j])], vt.at[k, band(g), at(far[j])], v_s.at[0], vp_r.at[g, j], peer)

    def v_out(m):
        return pltpu.make_async_copy(vst.at[at(m)], vec_hbm.at[place(m, x)], v_s.at[2])

    def write_out(m):
        for side in range(2):
            @pl.when(x == side)
            def _():
                block = [vt[k, dst : dst + n, at(m)] for _, dst, n in sorted(pieces(0, side))]
                vst[at(m), :] = jnp.concatenate(block, axis=0).T
        v_out(m).start()

    def weigh(rows):
        tw[0, rows, :] = dot3(halves(wf[1, rows, :]), halves(tb[0]), NT)

    def finish(rows, m):
        vt[k, rows, at(m)] = xt[rows, at(m)] - dot3(halves(tw[0, rows, :]), halves(y1b[at(m), :]), NT)

    a1.finish()
    weigh(band(0))
    for j, m in enumerate(sent):
        finish(band(0), m)
        v_peer(0, j).start()
    a2.finish()
    weigh(later)
    for j, m in enumerate(sent):
        finish(later, m)
        v_peer(1, j).start()
    for g in range(2, len(parts)):
        for j in range(len(sent)):
            v_peer(g, j).start()
    everything = pl.ds(0, wide)
    for m in sent:
        v_mate(0, everything, m).start()
    for m in kept:
        finish(everything, m)
        v_mate(0, everything, m).start()
    for m in late:
        take(m)
    for m in early:
        wait_y(0, m)
        finish(everything, m)
        v_mate(0, everything, m).start()

    def multiply(m):
        v_mate(0, everything, m).wait_recv()
        right = halves(sb[:, place(m, x)])
        for h in range(2):
            pt[h] += dot3(halves(vt[h, :, at(m)]), right, NT)

    for m in sent + kept:
        multiply(m)
    for m in late:
        extra_inner(m)
        wait_y(0, m)
        finish(everything, m)
        v_mate(0, everything, m).start()
    for m in extras:
        multiply(m)

    def multiply_far(g, j):
        m = far[j]
        cut = slice(m[0] - reach, m[0] - reach + m[1])
        both = vt[:, band(g), at(m)].reshape(2 * spans[g][1], m[1])
        added = dot3(halves(both), (far_h[:, cut], far_l[:, cut]), NT)
        pt[:, band(g), :] += added.reshape(2, spans[g][1], pt.shape[2])

    def scatter(g):
        n = parts[g]

        def piece(zz, yy):
            start = spans[g][0] + ((zz // 2) * per + yy) * n
            return pt.at[lax.rem(zz, 2), pl.ds(pl.multiple_of(start, 8), n)]

        def rows(ref):
            return lambda d: ref.at[d, pl.ds(offs[g], n)]

        return Sum(3 + g, piece, rows(pyb), rows(pzb), lambda count: sb.at[pl.ds(0, count * n), pl.ds(0, pt.shape[2])])

    def collect(g):
        out_ref[offs[g] : offs[g] + parts[g], :] = last[g].total()

    last = []
    todo = [(g, j) for g in range(len(parts)) for j in range(len(sent))]

    def arrived(g, j):
        v_mate(g, band(g), far[j]).wait_recv()
        multiply_far(g, j)
        if j == len(sent) - 1:
            last.append(scatter(g))
        elif g and j == len(sent) - 2 and g < len(parts) - 1:
            last[g - 1].relay()

    for t, (g, j) in enumerate(todo):
        v_peer(g, j).wait_recv()
        v_mate(g, band(g), far[j]).start()
        if t:
            arrived(*todo[t - 1])
        if t < len(locals_):
            write_out(locals_[t])
    arrived(*todo[-1])
    for m in locals_[len(todo):]:
        write_out(m)
    for one in last[:-1]:
        one.relay()
    for m in far:
        write_out(m)
    last[-1].relay()
    for g in range(len(parts) - 1):
        collect(g)
    for s in (a0, a1, a2):
        s.drain()
    sent_all(x_hbm.at[pl.ds(0, held)], bulk_s.at[0])
    for i in (1, 2, 3):
        sent_all(y_hbm.at[:, pl.ds(0, held)], bulk_s.at[i])
    sent_all(vt.at[0, :, pl.ds(0, sum(n for _, n in sent))], v_s.at[0])
    sent_all(vt.at[0], v_s.at[1])
    pltpu.make_async_copy(vst, vec_hbm, v_s.at[2]).wait()
    collect(len(parts) - 1)
    for done in last:
        done.drain()


CUTS = 2
CHUNK = 4
AHEAD = 3
EARLY = (4,)
LATE = (2,)
PARTS = (2, 1, 1)
UNITS = 16
VMEM_BYTES = 54_000_000


def on_grid(nrow, ncol, eigvecs, reflectors, factors, slab):
    size, bw = eigvecs.shape
    panel = factors.shape[1]
    nz = nrow // 2
    half = size // 2
    unit = half // UNITS
    q = CHUNK * unit
    nq = half // q

    def ranges(start, sizes):
        out = []
        for n in sizes:
            out.append((start, n * unit))
            start += n * unit
        return out

    early = ranges(half, EARLY)
    late = ranges(half + sum(n for _, n in early), LATE)
    extra = sum(EARLY) + sum(LATE)
    kept = ranges(0, (extra,))
    rest = (UNITS - extra) % CHUNK
    sent = ranges(extra * unit, (CHUNK,) * ((UNITS - extra) // CHUNK) + ((rest,) if rest else ()))
    held = half + extra * unit
    away = half - extra * unit
    wide = 2 * bw
    f32 = jnp.float32
    rows = wide // nrow
    mine = slab.shape[0]
    share = ncol * bw // nrow
    parts = tuple(n * share // sum(PARTS) for n in PARTS)
    g = len(parts)
    chunks = nq + len(EARLY) + len(LATE)
    slots = (1 + g) * len(sent) + len(kept) + len(EARLY) + len(LATE)
    sem = pltpu.SemaphoreType.DMA
    vmem = pltpu.VMEM
    vectors, product = pl.pallas_call(
        functools.partial(whole_kernel, (nz, q, nq, AHEAD, early, late, kept, sent, parts)),
        out_shape=(
            jax.ShapeDtypeStruct((size, bw), f32),
            jax.ShapeDtypeStruct((share, mine), f32),
        ),
        in_specs=[pl.BlockSpec(memory_space=pltpu.HBM)] * 4,
        out_specs=(pl.BlockSpec(memory_space=pl.ANY), pl.BlockSpec(memory_space=pltpu.VMEM)),
        scratch_shapes=[
            vmem((held, wide), f32), vmem((wide, held), f32), vmem((held, panel), f32), vmem((held, panel), f32),
            vmem(slab.shape, f32), vmem((mine, away), jnp.bfloat16), vmem((mine, away), jnp.bfloat16),
            vmem(factors.shape, f32), vmem((2, wide, size), f32), vmem((size, bw), f32),
            vmem((2, wide, panel), f32), vmem((panel, panel), f32),
            vmem((2, wide, panel), f32), vmem((2, wide, panel), f32),
            vmem((2, nz, rows, panel), f32), vmem((2, nz, rows, panel), f32),
            vmem((2, rows, panel), f32), vmem((2, rows, panel), f32),
            vmem((2, wide, mine), f32),
            vmem((nz, share, mine), f32), vmem((nz, share, mine), f32),
            sem((2,)), sem((4,)), sem((chunks,)), sem((2, chunks)), sem((2, chunks)),
            sem((3 + g, nz)), sem((3 + g,)), sem((3 + g,)), sem((3,)), sem((3,)),
            sem((3, nz)), sem((3,)), sem((3,)), sem((g, len(sent))), sem((slots,)), sem((3,)),
        ],
        compiler_params=pltpu.CompilerParams(
            collective_id=0, has_side_effects=True, vmem_limit_bytes=VMEM_BYTES),
        name="whole",
    )(eigvecs, reflectors, factors, slab)
    return vectors, product.T


def on_any(nrow, ncol, eigvecs, reflectors, factors, slab):
    c = lax.axis_index("col")
    first_own, second_own = reflectors[0], reflectors[1]
    all_x, second_y, first_y = (
        lax.all_gather(block, "col", axis=1, tiled=True) for block in (eigvecs, second_own, first_own)
    )
    own = second_own.shape[1]
    both = jnp.concatenate([second_own, first_own], axis=1)
    stacked = jnp.concatenate([tdot(both, all_x), tdot(first_own, second_y)])
    slab_x, slab_second, slab_first = (dot(block, slab, ((0,), (1,))) for block in (all_x, second_y, first_y))
    sums = lax.all_gather(lax.psum(stacked, "row"), "col")
    panel = factors.shape[1]
    second_w, first_raw, gram = (sums[:, i * own : (i + 1) * own].reshape(panel, -1) for i in range(3))
    second_tw = dot(factors[1], second_w)
    first_tw = dot(factors[0], first_raw - dot(gram, second_tw))
    partial = slab_x - tdot(second_tw, slab_second) - tdot(first_tw, slab_first)
    product = lax.psum_scatter(partial, "row", tiled=True)
    vectors = eigvecs
    for block, tw in ((second_y, second_tw), (first_y, first_tw)):
        width = eigvecs.shape[1]
        vectors = vectors - dot(block, lax.dynamic_slice_in_dim(tw, c * width, width, axis=1))
    return vectors, product.T


def solution(mesh):
    nrow, ncol = mesh.shape["row"], mesh.shape["col"]
    fits = ncol == 4 and nrow == 2 * ncol
    return jax.shard_map(
        functools.partial(on_grid if fits else on_any, nrow, ncol),
        mesh=mesh,
        in_specs=(P("row", "col"), P(None, "row", "col"), P(), P("col", "row")),
        out_specs=(P("row", "col"), P("col", "row")),
        check_vma=False,
    )
```

```python
import functools

import jax
import jax.numpy as jnp
from jax import lax
from jax.experimental import pallas as pl
from jax.experimental.pallas import tpu as pltpu
from jax.sharding import PartitionSpec as P

MESH = pl.DeviceIdType.MESH
NN = ((1,), (0,))
NT = ((1,), (1,))
TN = ((0,), (0,))


def dot(left, right, dims=NN):
    return lax.dot_general(
        left, right, (dims, ((), ())), precision=lax.Precision.HIGH, preferred_element_type=jnp.float32
    )


def tdot(left, right):
    return dot(left, right, TN)


def halves(a):
    high = a.astype(jnp.bfloat16)
    return high, (a - high.astype(jnp.float32)).astype(jnp.bfloat16)


def dot3(left, right, dims):
    def one(a, b):
        return lax.dot_general(a, b, (dims, ((), ())), preferred_element_type=jnp.float32)

    (lh, ll), (rh, rl) = left, right
    free = 1 - dims[0][0]
    size = lh.shape[free]
    if size > STACK:
        return one(lh, rh) + (one(lh, rl) + one(ll, rh))
    stacked = one(jnp.concatenate([lh, ll], axis=free), rh)
    return stacked[:size] + (one(lh, rl) + stacked[size:])


STACK = 256


def whole_kernel(
    plan, x_hbm, y_hbm, t_hbm, s_hbm, vec_hbm, out_ref,
    xb, xt, y1b, y2b, sb, far_h, far_l, tb, vt, vst, w, gram, wf, tw, ybuf, zbuf, xs, xr, pt, pyb, pzb,
    ls, bulk_s, x_r, y_r, py_r, ry_r, rz_r, r_s, rx_s, rx_r, gz_r, gy_r, g_s, vp_r, vm_r, v_s,
):
    nz, q, nq, ahead, early, late, kept, sent, parts = plan
    half = nq * q
    must = [(i * q, q) for i in range(nq)]
    extras = early + late
    held = half + sum(n for _, n in extras)
    bw = x_hbm.shape[1]
    share = out_ref.shape[0]
    per = bw // share
    offs = [sum(parts[:g]) for g in range(len(parts))]
    spans = [(2 * per * o, 2 * per * n) for o, n in zip(offs, parts)]
    first_span = spans[0][1]
    wide = xt.shape[0]
    r, c = lax.axis_index("row"), lax.axis_index("col")
    z, y = r // 2, lax.rem(r, 2)
    x, k = c // 2, lax.rem(c, 2)
    mate = (r, c + 1 - 2 * k)
    peer = (r, c + 2 - 4 * x)
    peer_block = c + 2 - 4 * x
    ynext = (r + 1 - 2 * y, c)

    def zat(d):
        return lax.rem(z + d, nz)

    def znext(d):
        return (zat(d) * 2 + y, c)

    partners = [mate, peer, ynext] + [znext(d) for d in range(1, nz)]
    barrier = pltpu.get_barrier_semaphore()
    for other in partners:
        pl.semaphore_signal(barrier, inc=1, device_id=other, device_id_type=MESH)
    pl.semaphore_wait(barrier, len(partners))

    def send(src, dst, s, t, device):
        return pltpu.make_async_remote_copy(src, dst, s, t, device_id=device, device_id_type=MESH)

    def sent_all(ref, s):
        send(ref, ref, s, s, mate).wait_send()

    def arrive(ref, s):
        send(ref, ref, s, s, mate).wait_recv()

    def at(m):
        return pl.ds(m[0], m[1])

    def place(m, side):
        start, size = m
        base = side * half + start if start < half else (1 - side) * half + start - half
        return pl.ds(pl.multiple_of(base, 128), size)

    def lanes(b):
        return pl.ds(pl.multiple_of(b * bw, bw), bw)

    def index(m):
        return m[0] // q if m[0] < half else nq + extras.index(m)

    panels = (y1b, y2b)

    def x_local(m):
        return pltpu.make_async_copy(x_hbm.at[place(m, x)], xb.at[at(m), lanes(x)], x_r.at[index(m)])

    def x_peer(m, slot):
        return send(x_hbm.at[place(m, 1 - x)], xb.at[at(m), lanes(x)], bulk_s.at[0], x_r.at[slot], peer)

    def y_local(p, m):
        return pltpu.make_async_copy(
            y_hbm.at[p, place(m, x)], panels[p].at[at(m), lanes(c)], y_r.at[p, index(m)])

    def y_peer(p, m, slot):
        return send(
            y_hbm.at[p, place(m, 1 - x)], panels[p].at[at(m), lanes(c)], bulk_s.at[1], py_r.at[p, slot], peer)

    def y_mate(p, m):
        return send(
            y_hbm.at[p, place(m, x)], panels[p].at[at(m), lanes(c)], bulk_s.at[2], y_r.at[p, index(m)], mate)

    def y_forward(p, m):
        block = panels[p].at[at(m), lanes(peer_block)]
        return send(block, block, bulk_s.at[3], y_r.at[p, index(m)], mate)

    def wait_y(p, m):
        block = panels[p].at[at(m), pl.ds(0, 3 * bw)]
        pltpu.make_async_copy(block, block, y_r.at[p, index(m)]).wait()

    def pass_on(p, m):
        y_peer(p, m, index(m)).wait_recv()
        y_forward(p, m).start()

    def cut(m):
        n = m[1] // CUTS
        return [(m[0] + i * n, n) for i in range(CUTS)]

    def send_x(m):
        for part in cut(m):
            x_peer(part, index(m)).start()

    def send_y(p, m):
        for part in cut(m):
            y_peer(p, part, index(m)).start()

    def send_bulk(m):
        send_x(m)
        send_y(1, m)
        send_y(0, m)

    for m in must:
        send_x(m)
        send_y(1, m)
    for m in must[:ahead]:
        send_y(0, m)
    for m in must + extras:
        x_local(m).start()
        for p in (1, 0):
            y_mate(p, m).start()
            y_local(p, m).start()
    t_copy = pltpu.make_async_copy(t_hbm, tb, ls.at[0])
    s_copy = pltpu.make_async_copy(s_hbm, sb, ls.at[1])
    t_copy.start()
    s_copy.start()

    w[...] = jnp.zeros_like(w)
    gram[...] = jnp.zeros_like(gram)
    pt[...] = jnp.zeros_like(pt)
    t_copy.wait()
    s_copy.wait()
    far = [(start + half, size) for start, size in sent]
    reach = far[0][0]
    for m in far:
        high, low = halves(sb[:, place(m, x)])
        far_h[:, m[0] - reach : m[0] - reach + m[1]] = high
        far_l[:, m[0] - reach : m[0] - reach + m[1]] = low

    def pieces(block, side):
        for o, n, (base, _) in zip(offs, parts, spans):
            for h in range(per):
                yield block + h * share + o, base + (side * per + h) * n, n

    def turn(m):
        pltpu.make_async_copy(xb.at[at(m)], xb.at[at(m)], x_r.at[index(m)]).wait()
        turned = xb[at(m), :].T
        for side in range(2):
            for src, dst, n in pieces(side * bw, side):
                xt[dst : dst + n, at(m)] = turned[src : src + n]

    def begin(m):
        turn(m)
        wait_y(1, m)
        w[0] += dot3(halves(xt[:, at(m)]), halves(y2b[at(m), :]), NN)

    for i, m in enumerate(must):
        pass_on(1, m)
        if i:
            begin(must[i - 1])
    begin(must[-1])

    class Sum:
        def __init__(self, n, piece, ys, zs, whole):
            self.n, self.piece, self.ys, self.zs, self.whole = n, piece, ys, zs, whole
            self.pending = list(range(1, nz))
            self.out = [
                send(piece(zat(d), 1 - y), ys(d), r_s.at[n], ry_r.at[n, d], ynext) for d in self.pending + [0]]
            self.hops = [send(piece(zat(d), y), zs(d), r_s.at[n], rz_r.at[n], znext(d)) for d in range(1, nz)]
            for copy in self.out:
                copy.start()

        def relay(self, count=nz):
            for d in self.pending[:count]:
                self.out[d - 1].wait_recv()
                self.piece(zat(d), y)[...] += self.ys(d)[...]
                self.hops[d - 1].start()
            self.pending = self.pending[count:]

        def total(self):
            self.out[-1].wait_recv()
            total = self.piece(z, y)[...] + self.ys(0)[...]
            arrive(self.whole(nz - 1), rz_r.at[self.n])
            for d in range(1, nz):
                total = total + self.zs(d)[...]
            return total

        def drain(self):
            sent_all(self.whole(2 * nz - 1), r_s.at[self.n])

    class AllSum:
        def __init__(self, n, panel, base, size):
            self.n = n
            rows = size // (2 * nz)
            self.rows = pl.ds(base // (2 * nz), rows)

            def block(ref, zz, yy):
                return ref.at[panel, pl.ds(pl.multiple_of(base + (zz * 2 + yy) * rows, 8), rows)]

            self.final = lambda zz, yy: block(wf, zz, yy)
            self.whole = lambda count: w.at[panel, pl.ds(0, count * rows)]
            self.panel = panel
            self.sum = Sum(
                n, lambda zz, yy: block(w, zz, yy),
                lambda d: ybuf.at[panel, d, self.rows], lambda d: zbuf.at[panel, d, self.rows], self.whole)
            self.relay = self.sum.relay

        def swap(self):
            n = self.n
            mine, other = xs.at[self.panel, self.rows], xr.at[self.panel, self.rows]
            mine[...] = self.sum.total()
            self.swapped = send(mine, other, rx_s.at[n], rx_r.at[n], peer)
            self.swapped.start()

        def gather(self):
            n = self.n
            self.swapped.wait_recv()
            mine = self.final(z, y)
            mine[...] = xs[self.panel, self.rows] + xr[self.panel, self.rows]
            self.along = [send(mine, mine, g_s.at[n], gz_r.at[n, d], znext(d)) for d in range(1, nz)]
            for copy in self.along:
                copy.start()
            self.across = [send(mine, mine, g_s.at[n], gy_r.at[n], ynext)]
            self.across[0].start()

        def forward(self):
            for d in range(1, nz):
                self.along[d - 1].wait_recv()
                block = self.final(lax.rem(z + nz - d, nz), y)
                self.across.append(send(block, block, g_s.at[self.n], gy_r.at[self.n], ynext))
                self.across[-1].start()

        def finish(self):
            arrive(self.whole(nz), gy_r.at[self.n])

        def drain(self):
            self.sum.drain()
            self.swapped.wait_send()
            sent_all(self.whole(2 * nz - 1), g_s.at[self.n])

    def inner(m):
        xt[:, at(m)] = xt[:, at(m)] - dot3(halves(tw[1]), halves(y2b[at(m), :]), NT)

    def raw(m):
        wait_y(0, m)
        first = halves(y1b[at(m), :])
        w[1] += dot3(halves(xt[:, at(m)]), first, NN)
        gram[...] += dot3(halves(y2b[at(m), :]), first, TN)

    a0 = AllSum(0, 0, 0, wide)
    a0.relay()
    a0.swap()
    for m in must[ahead:]:
        send_y(0, m)
    for m in early:
        send_bulk(m)
    for m in must[:-2]:
        pass_on(0, m)
    for m in must[:-2]:
        raw(m)
    a0.gather()
    pass_on(0, must[-2])
    raw(must[-2])
    a0.forward()
    pass_on(0, must[-1])
    raw(must[-1])
    a0.finish()
    tw[1] = dot3(halves(wf[0]), halves(tb[1]), NT)
    w[1] = w[1] - dot3(halves(tw[1]), halves(gram[...]), NN)

    def take(m):
        pass_on(1, m)
        pass_on(0, m)

    def extra_inner(m):
        turn(m)
        wait_y(1, m)
        inner(m)

    a1 = AllSum(1, 1, 0, first_span)
    a2 = AllSum(2, 1, first_span, wide - first_span)
    a1.relay()
    for m in must[:2]:
        inner(m)
    a2.relay()
    a1.swap()
    a2.swap()
    for m in late:
        send_bulk(m)
    for m in must[2:]:
        inner(m)
    a1.gather()
    a2.gather()
    for m in early:
        take(m)
    a1.forward()
    a2.forward()
    for m in early:
        extra_inner(m)

    def band(g):
        return pl.ds(*spans[g])

    later = pl.ds(first_span, wide - first_span)
    locals_ = sent + kept + extras

    def v_mate(b, rows, m):
        block = vt.at[k, rows, at(m)]
        slot = locals_.index(m) if m in locals_ else len(locals_) + b * len(far) + far.index(m)
        return send(block, block, v_s.at[1], vm_r.at[slot], mate)

    def v_peer(g, j):
        return send(vt.at[k, band(g), at(sent[j])], vt.at[k, band(g), at(far[j])], v_s.at[0], vp_r.at[g, j], peer)

    def v_out(m):
        return pltpu.make_async_copy(vst.at[at(m)], vec_hbm.at[place(m, x)], v_s.at[2])

    def write_out(m):
        for side in range(2):
            @pl.when(x == side)
            def _():
                block = [vt[k, dst : dst + n, at(m)] for _, dst, n in sorted(pieces(0, side))]
                vst[at(m), :] = jnp.concatenate(block, axis=0).T
        v_out(m).start()

    def weigh(rows):
        tw[0, rows, :] = dot3(halves(wf[1, rows, :]), halves(tb[0]), NT)

    def finish(rows, m):
        vt[k, rows, at(m)] = xt[rows, at(m)] - dot3(halves(tw[0, rows, :]), halves(y1b[at(m), :]), NT)

    a1.finish()
    weigh(band(0))
    for j, m in enumerate(sent):
        finish(band(0), m)
        v_peer(0, j).start()
    a2.finish()
    weigh(later)
    for j, m in enumerate(sent):
        finish(later, m)
        v_peer(1, j).start()
    for g in range(2, len(parts)):
        for j in range(len(sent)):
            v_peer(g, j).start()
    everything = pl.ds(0, wide)
    for m in sent:
        v_mate(0, everything, m).start()
    for m in kept:
        finish(everything, m)
        v_mate(0, everything, m).start()
    for m in late:
        take(m)
    for m in early:
        wait_y(0, m)
        finish(everything, m)
        v_mate(0, everything, m).start()

    def multiply(m):
        v_mate(0, everything, m).wait_recv()
        right = halves(sb[:, place(m, x)])
        for h in range(2):
            pt[h] += dot3(halves(vt[h, :, at(m)]), right, NT)

    for m in sent + kept:
        multiply(m)
    for m in late:
        extra_inner(m)
        wait_y(0, m)
        finish(everything, m)
        v_mate(0, everything, m).start()
    for m in extras:
        multiply(m)

    def multiply_far(g, j):
        m = far[j]
        cut = slice(m[0] - reach, m[0] - reach + m[1])
        both = vt[:, band(g), at(m)].reshape(2 * spans[g][1], m[1])
        added = dot3(halves(both), (far_h[:, cut], far_l[:, cut]), NT)
        pt[:, band(g), :] += added.reshape(2, spans[g][1], pt.shape[2])

    def scatter(g):
        n = parts[g]

        def piece(zz, yy):
            start = spans[g][0] + ((zz // 2) * per + yy) * n
            return pt.at[lax.rem(zz, 2), pl.ds(pl.multiple_of(start, 8), n)]

        def rows(ref):
            return lambda d: ref.at[d, pl.ds(offs[g], n)]

        return Sum(3 + g, piece, rows(pyb), rows(pzb), lambda count: sb.at[pl.ds(0, count * n), pl.ds(0, pt.shape[2])])

    def collect(g):
        out_ref[offs[g] : offs[g] + parts[g], :] = last[g].total()

    last = []
    todo = [(g, j) for g in range(len(parts)) for j in range(len(sent))]

    def arrived(g, j):
        v_mate(g, band(g), far[j]).wait_recv()
        multiply_far(g, j)
        if j == len(sent) - 1:
            last.append(scatter(g))
        elif g and j == len(sent) - 2 and g < len(parts) - 1:
            last[g - 1].relay()

    for t, (g, j) in enumerate(todo):
        v_peer(g, j).wait_recv()
        v_mate(g, band(g), far[j]).start()
        if t:
            arrived(*todo[t - 1])
        if t < len(locals_):
            write_out(locals_[t])
    arrived(*todo[-1])
    for m in locals_[len(todo):]:
        write_out(m)
    for one in last[:-1]:
        one.relay()
    for m in far:
        write_out(m)
    last[-1].relay()
    for g in range(len(parts) - 1):
        collect(g)
    for s in (a0, a1, a2):
        s.drain()
    sent_all(x_hbm.at[pl.ds(0, held)], bulk_s.at[0])
    for i in (1, 2, 3):
        sent_all(y_hbm.at[:, pl.ds(0, held)], bulk_s.at[i])
    sent_all(vt.at[0, :, pl.ds(0, sum(n for _, n in sent))], v_s.at[0])
    sent_all(vt.at[0], v_s.at[1])
    pltpu.make_async_copy(vst, vec_hbm, v_s.at[2]).wait()
    collect(len(parts) - 1)
    for done in last:
        done.drain()


CUTS = 2
CHUNK = 4
AHEAD = 3
EARLY = (4,)
LATE = (2,)
PARTS = (2, 1, 1)
UNITS = 16
VMEM_BYTES = 54_000_000


def on_grid(nrow, ncol, eigvecs, reflectors, factors, slab):
    size, bw = eigvecs.shape
    panel = factors.shape[1]
    nz = nrow // 2
    half = size // 2
    unit = half // UNITS
    q = CHUNK * unit
    nq = half // q

    def ranges(start, sizes):
        out = []
        for n in sizes:
            out.append((start, n * unit))
            start += n * unit
        return out

    early = ranges(half, EARLY)
    late = ranges(half + sum(n for _, n in early), LATE)
    extra = sum(EARLY) + sum(LATE)
    kept = ranges(0, (extra,))
    rest = (UNITS - extra) % CHUNK
    sent = ranges(extra * unit, (CHUNK,) * ((UNITS - extra) // CHUNK) + ((rest,) if rest else ()))
    held = half + extra * unit
    away = half - extra * unit
    wide = 2 * bw
    f32 = jnp.float32
    rows = wide // nrow
    mine = slab.shape[0]
    share = ncol * bw // nrow
    parts = tuple(n * share // sum(PARTS) for n in PARTS)
    g = len(parts)
    chunks = nq + len(EARLY) + len(LATE)
    slots = (1 + g) * len(sent) + len(kept) + len(EARLY) + len(LATE)
    sem = pltpu.SemaphoreType.DMA
    vmem = pltpu.VMEM
    vectors, product = pl.pallas_call(
        functools.partial(whole_kernel, (nz, q, nq, AHEAD, early, late, kept, sent, parts)),
        out_shape=(
            jax.ShapeDtypeStruct((size, bw), f32),
            jax.ShapeDtypeStruct((share, mine), f32),
        ),
        in_specs=[pl.BlockSpec(memory_space=pltpu.HBM)] * 4,
        out_specs=(pl.BlockSpec(memory_space=pl.ANY), pl.BlockSpec(memory_space=pltpu.VMEM)),
        scratch_shapes=[
            vmem((held, wide), f32), vmem((wide, held), f32), vmem((held, panel), f32), vmem((held, panel), f32),
            vmem(slab.shape, f32), vmem((mine, away), jnp.bfloat16), vmem((mine, away), jnp.bfloat16),
            vmem(factors.shape, f32), vmem((2, wide, size), f32), vmem((size, bw), f32),
            vmem((2, wide, panel), f32), vmem((panel, panel), f32),
            vmem((2, wide, panel), f32), vmem((2, wide, panel), f32),
            vmem((2, nz, rows, panel), f32), vmem((2, nz, rows, panel), f32),
            vmem((2, rows, panel), f32), vmem((2, rows, panel), f32),
            vmem((2, wide, mine), f32),
            vmem((nz, share, mine), f32), vmem((nz, share, mine), f32),
            sem((2,)), sem((4,)), sem((chunks,)), sem((2, chunks)), sem((2, chunks)),
            sem((3 + g, nz)), sem((3 + g,)), sem((3 + g,)), sem((3,)), sem((3,)),
            sem((3, nz)), sem((3,)), sem((3,)), sem((g, len(sent))), sem((slots,)), sem((3,)),
        ],
        compiler_params=pltpu.CompilerParams(
            collective_id=0, has_side_effects=True, vmem_limit_bytes=VMEM_BYTES),
        name="whole",
    )(eigvecs, reflectors, factors, slab)
    return vectors, product.T


def on_any(nrow, ncol, eigvecs, reflectors, factors, slab):
    c = lax.axis_index("col")
    first_own, second_own = reflectors[0], reflectors[1]
    all_x, second_y, first_y = (
        lax.all_gather(block, "col", axis=1, tiled=True) for block in (eigvecs, second_own, first_own)
    )
    own = second_own.shape[1]
    both = jnp.concatenate([second_own, first_own], axis=1)
    stacked = jnp.concatenate([tdot(both, all_x), tdot(first_own, second_y)])
    slab_x, slab_second, slab_first = (dot(block, slab, ((0,), (1,))) for block in (all_x, second_y, first_y))
    sums = lax.all_gather(lax.psum(stacked, "row"), "col")
    panel = factors.shape[1]
    second_w, first_raw, gram = (sums[:, i * own : (i + 1) * own].reshape(panel, -1) for i in range(3))
    second_tw = dot(factors[1], second_w)
    first_tw = dot(factors[0], first_raw - dot(gram, second_tw))
    partial = slab_x - tdot(second_tw, slab_second) - tdot(first_tw, slab_first)
    product = lax.psum_scatter(partial, "row", tiled=True)
    vectors = eigvecs
    for block, tw in ((second_y, second_tw), (first_y, first_tw)):
        width = eigvecs.shape[1]
        vectors = vectors - dot(block, lax.dynamic_slice_in_dim(tw, c * width, width, axis=1))
    return vectors, product.T


def solution(mesh):
    nrow, ncol = mesh.shape["row"], mesh.shape["col"]
    fits = ncol == 4 and nrow == 2 * ncol
    return jax.shard_map(
        functools.partial(on_grid if fits else on_any, nrow, ncol),
        mesh=mesh,
        in_specs=(P("row", "col"), P(None, "row", "col"), P(), P("col", "row")),
        out_specs=(P("row", "col"), P("col", "row")),
        check_vma=False,
    )
```
